32 devices in a mesh: grp: 4 (over y, x), dev: 8 (over z, core).
Axes of the slice: x: 2, y: 2, z: 4, core: 2. Of those that a mesh axis runs over, the one named last changes fastest.
Arguments:
- obs_coord: float32 [3, 131072], P(None, ('grp', 'dev')), may hold values from -1 to 1
- obs_resid: float32 [131072], P(('grp', 'dev')), may hold values from -6 to 6
- obs_weight: float32 [131072], P(('grp', 'dev')), may hold values from 0.5 to 2
- obs_dest: int32 [131072], P(('grp', 'dev')), may hold values from 0 to 7, as said below
- obs_send_slot: int32 [131072], P(('grp', 'dev')), may hold values from 0 to 1023, as said below
- obs_elem: int32 [131072], P(('grp', 'dev')), may hold values from 0 to 255, as said below
- obs_slot: int32 [131072], P(('grp', 'dev')), may hold values from 0 to 31, as said below
Outputs:
- nodal: float32 [16, 64, 8, 512], P('grp', 'dev')
- total_cost: float32 [], replicated
The draws below stay inside these ranges and needn't reach their ends.
Inputs may be any that keep to these rules, and one draw needn't show every extreme that they name: `obs_dest`: from the rows of one device, at most 1024 observations go to any one destination; in every group one destination receives exactly 1024 from every device of the group. `obs_send_slot`: distinct among the rows of one device with the same obs_dest. `obs_elem`: together with obs_slot distinct among all observations of a group with the same obs_dest. `obs_slot`: on every destination some element uses all 32 slots.
All inputs are finite; a program needn't handle non-finite values.
Results may differ from the reference program's by a relative error of at most 0.00017.
Values sent between devices are 32-bit elements; how exact they have to be, the bound alone decides.
A program may use at most 64 MiB of HBM per device.

```python
import math
import jax
import jax.numpy as jnp
from jax import lax

OBS_DEV = 4096
EX = 4
EY = 8
EZ = 8
ELEM_DEV = 256
CAP = 1024
SLOTS = 32
TOTAL_OBS = 131072
NEX = 16
NEY = 64
N_GRP = 4
N_DEV = 8


def layout(key):
    peer_count = 2 * OBS_DEV // CAP
    group_count = TOTAL_OBS // (OBS_DEV * peer_count)
    cell_count = ELEM_DEV * SLOTS
    key_a, key_b, key_c, key_d, key_e = jax.random.split(key, 5)
    columns = jnp.arange(cell_count, dtype=jnp.int32)
    wanted = columns // CAP
    favored = jax.random.randint(key_a, (group_count, 1, 1), 0, peer_count, dtype=jnp.int32)
    jitter = jax.random.randint(key_b, (group_count, peer_count, cell_count), 1, 32768, dtype=jnp.int32)
    ranking = jnp.where(wanted[None, None, :] == favored, 0, jitter) * cell_count + columns
    picked = jnp.argsort(ranking, axis=-1)[:, :, :OBS_DEV].astype(jnp.int32)
    target = wanted[picked]
    row_ids = jnp.arange(OBS_DEV, dtype=jnp.int32)
    shuffle_keys = jax.random.randint(key_c, (group_count, peer_count, OBS_DEV), 0, 32768, dtype=jnp.int32) * OBS_DEV + row_ids
    mixing = jnp.argsort(shuffle_keys, axis=-1).astype(jnp.int32)
    target = jnp.take_along_axis(target, mixing, axis=-1)
    sorter = jnp.argsort(target, axis=-1, stable=True).astype(jnp.int32)
    sorted_target = jnp.take_along_axis(target, sorter, axis=-1)
    steps_row = jnp.broadcast_to(row_ids, sorted_target.shape)
    change = jnp.concatenate([jnp.ones((group_count, peer_count, 1), bool), sorted_target[:, :, 1:] != sorted_target[:, :, :-1]], axis=-1)
    starts = lax.cummax(jnp.where(change, steps_row, 0), axis=2)
    ranks_sorted = steps_row - starts
    inverse = jnp.argsort(sorter, axis=-1).astype(jnp.int32)
    send_slot = jnp.take_along_axis(ranks_sorted, inverse, axis=-1)
    owner = jnp.arange(group_count * peer_count, dtype=jnp.int32).reshape(group_count, peer_count, 1)
    segment = (owner * peer_count + target).reshape(-1)
    counts = jax.ops.segment_sum(jnp.ones_like(segment), segment, num_segments=group_count * peer_count * peer_count)
    counts = counts.reshape(group_count, peer_count, peer_count)
    earlier = jnp.cumsum(counts, axis=1) - counts
    arrival = jnp.take_along_axis(earlier, target, axis=2) + send_slot
    favored_elem = jax.random.randint(key_d, (group_count, peer_count, 1), 0, ELEM_DEV, dtype=jnp.int32)
    jitter_two = jax.random.randint(key_e, (group_count, peer_count, cell_count), 1, 32768, dtype=jnp.int32)
    ranking_two = jnp.where((columns // SLOTS)[None, None, :] == favored_elem, 0, jitter_two) * cell_count + columns
    table = jnp.argsort(ranking_two, axis=-1).astype(jnp.int32)
    group_ids = jnp.arange(group_count, dtype=jnp.int32).reshape(group_count, 1, 1)
    flat_index = ((group_ids * peer_count + target) * cell_count + arrival).reshape(-1)
    chosen = table.reshape(-1)[flat_index]
    return (target.reshape(-1).astype(jnp.int32), send_slot.reshape(-1).astype(jnp.int32), (chosen // SLOTS).astype(jnp.int32), (chosen % SLOTS).astype(jnp.int32))


def draw_obs_dest(key, part):
    return layout(jax.random.fold_in(key, 11))[0]


def draw_obs_send_slot(key, part):
    return layout(jax.random.fold_in(key, 11))[1]


def draw_obs_elem(key, part):
    return layout(jax.random.fold_in(key, 11))[2]


def draw_obs_slot(key, part):
    return layout(jax.random.fold_in(key, 11))[3]


def block_levels(stream_key, dims, pieces, smallest, top_value):
    level, own = 1.0, jax.random.fold_in(stream_key, 6)
    for dim, parts in pieces:
        draws = jnp.exp(jax.random.uniform(jax.random.fold_in(own, dim), (parts,), jnp.float32, smallest / len(pieces), top_value / len(pieces)))
        level = level * jnp.repeat(draws, dims[dim] // parts).reshape([-1 if axis == dim else 1 for axis in range(len(dims))])
    return level


def gaussian(stream_key, shape, width, reach, cuts=(), kind=jnp.bfloat16):
    loudness = block_levels(stream_key, shape, cuts, -0.22, 0.18) if cuts else 1.0
    array = jax.random.normal(stream_key, shape, jnp.float32) * width * loudness
    return jnp.minimum(jnp.maximum(array, -reach), reach).astype(kind)


def setup_inputs(seed: int = 0) -> dict:
    keys = jax.random.split(jax.random.key(seed), 8)
    obs_coord = jnp.clip(jax.random.uniform(keys[0], (3, TOTAL_OBS), jnp.float32, -1.0, 1.0) * block_levels(keys[0], (3, TOTAL_OBS), ((1, 32),), -0.4, 0.0), -1.0, 1.0)
    obs_resid = gaussian(keys[1], (TOTAL_OBS,), 1.0, 6.0, ((0, 32),), jnp.float32)
    obs_weight = jnp.clip(jnp.exp(math.log(2.0) - 1.3862944 * jax.random.uniform(keys[2], (TOTAL_OBS,), jnp.float32) ** block_levels(keys[2], (TOTAL_OBS,), ((0, 32),), -0.2, 0.2)), 0.5, 2.0)
    obs_dest = draw_obs_dest(jax.random.fold_in(keys[7], 71), 0)
    obs_send_slot = draw_obs_send_slot(jax.random.fold_in(keys[7], 71), 0)
    obs_elem = draw_obs_elem(jax.random.fold_in(keys[7], 71), 0)
    obs_slot = draw_obs_slot(jax.random.fold_in(keys[7], 71), 0)
    return {"obs_coord": obs_coord, "obs_resid": obs_resid, "obs_weight": obs_weight, "obs_dest": obs_dest, "obs_send_slot": obs_send_slot, "obs_elem": obs_elem, "obs_slot": obs_slot}


def basis_values(position):
    anchors = [-math.cos(math.pi * k / 7) for k in range(8)]
    basis = []
    for node_i in range(8):
        factor = jnp.ones_like(position)
        for node_m in range(8):
            if node_m != node_i:
                factor = factor * ((position - anchors[node_m]) / (anchors[node_i] - anchors[node_m]))
        basis.append(factor)
    return jnp.stack(basis)


def contract(first_w, second_w, third_w):
    outer = (first_w[:, None, :] * second_w[None, :, :]).reshape(64, ELEM_DEV, SLOTS)
    third = third_w.reshape(8, ELEM_DEV, SLOTS)
    mixed = jnp.einsum("aes,kes->eak", outer, third, precision=lax.Precision.HIGHEST)
    return mixed.reshape(ELEM_DEV, 512)


def combine(field, elem_dim, node_dim, from_low, from_high):
    count = field.shape[elem_dim]
    low_plane = lax.slice_in_dim(field, 0, 1, axis=node_dim)
    high_plane = lax.slice_in_dim(field, 7, 8, axis=node_dim)
    after = jnp.concatenate([lax.slice_in_dim(low_plane, 1, count, axis=elem_dim), from_high], axis=elem_dim)
    before = jnp.concatenate([from_low, lax.slice_in_dim(high_plane, 0, count - 1, axis=elem_dim)], axis=elem_dim)
    middle = lax.slice_in_dim(field, 1, 7, axis=node_dim)
    return jnp.concatenate([low_plane + before, middle, high_plane + after], axis=node_dim)


def block_nodes(block):
    first_w = basis_values(block[0]) * block[3]
    return contract(first_w, basis_values(block[1]), basis_values(block[2]))


def reference(obs_coord, obs_resid, obs_weight, obs_dest, obs_send_slot, obs_elem, obs_slot):
    forcing = obs_weight * obs_resid
    total_cost = 0.5 * jnp.sum(forcing * obs_resid)
    cell_count = ELEM_DEV * SLOTS
    device_count = N_GRP * N_DEV
    source = jnp.arange(TOTAL_OBS, dtype=jnp.int32) // OBS_DEV
    group_index = source // N_DEV
    device = group_index * N_DEV + obs_dest
    position = device * cell_count + obs_elem * SLOTS + obs_slot
    values = jnp.concatenate([obs_coord, forcing[None, :]], axis=0)
    packed = jnp.zeros((4, device_count * cell_count), obs_coord.dtype).at[:, position].set(values)
    blocks = packed.reshape(4, device_count, cell_count).transpose(1, 0, 2)
    raw = lax.map(block_nodes, blocks)
    raw = raw.reshape(N_GRP, N_DEV, EX, EY, EZ, 512).transpose(0, 2, 1, 3, 4, 5)
    field = raw.reshape(NEX, NEY, EZ, 8, 8, 8)
    for elem_dim in range(3):
        node_dim = elem_dim + 3
        edge = lax.slice_in_dim(lax.slice_in_dim(field, 0, 1, axis=node_dim), 0, 1, axis=elem_dim)
        empty = jnp.zeros_like(edge)
        field = combine(field, elem_dim, node_dim, empty, empty)
    return field.reshape(NEX, NEY, EZ, 512), total_cost
```

```python
import functools
import math

import jax
import jax.numpy as jnp
from jax import lax
from jax.experimental import pallas as pl
from jax.experimental.pallas import tpu as pltpu
from jax.sharding import PartitionSpec as P

EX = 4
EY = 8
EZ = 8
ELEM_DEV = 256
LANES = 128
CHUNK = 1024
BATCHES = 4
MESH = pl.DeviceIdType.MESH
F32 = jnp.float32
BF16 = jnp.bfloat16

ANCHORS = [-math.cos(math.pi * k / 7) for k in range(8)]
OUTER_PAIRS = [(a, b) for a in (0, 7) for b in range(8)]
OUTER_PAIRS += [(a, b) for a in range(1, 7) for b in (0, 7)]
INNER_PAIRS = [(a, b) for a in range(1, 7) for b in range(1, 7)]
PAIRS = OUTER_PAIRS + INNER_PAIRS
COEFS = [
    1.0 / math.prod(ANCHORS[a] - ANCHORS[m] for m in range(8) if m != a) for a in range(8)
]


def basis_values(t):
    factors = [t - p for p in ANCHORS]
    prefix = [None] * 8
    suffix = [None] * 8
    for k in range(1, 8):
        prefix[k] = factors[k - 1] if k == 1 else prefix[k - 1] * factors[k - 1]
    for k in range(6, -1, -1):
        suffix[k] = factors[k + 1] if k == 6 else suffix[k + 1] * factors[k + 1]
    basis = []
    for a in range(8):
        if a == 0:
            product = suffix[0]
        elif a == 7:
            product = prefix[7]
        else:
            product = prefix[a] * suffix[a]
        basis.append(product * COEFS[a])
    return basis


def dot_nt(left, right):
    return lax.dot_general(left, right, (((1,), (1,)), ((), ())), preferred_element_type=F32)


def split2(value):
    first = value.astype(BF16).astype(F32)
    return first, (value - first).astype(BF16).astype(F32)


def one_hot(row, ids):
    tile = jnp.broadcast_to(row, (16, row.shape[1])).astype(BF16)
    hot = [jnp.where(part == tile, jnp.ones((), BF16), jnp.zeros((), BF16)) for part in ids]
    return hot[0] if len(hot) == 1 else jnp.concatenate(hot, axis=0)


def sublane_ids(count):
    ids = lax.broadcasted_iota(jnp.int32, (16, LANES), 0)
    return [(ids + 16 * i).astype(F32).astype(BF16) for i in range(count // 16)]


def kernel(
    dev_count, grp_count, capacity,
    coord_in, resid_in, weight_in, dest_in, slot_in, elem_in,
    out, cost,
    coord, resid, weight, dest, slot, elem, terms, left, lane_hot, send, recv,
    cost_send, cost_recv, group_send, group_recv,
    third, outer, product, onehot, raw, a_send, a_recv, b_send, b_recv, edge_recv,
    face_rows, inner_rows,
    send_sem, recv_sem, cost_send_sem, cost_recv_sem, group_send_sem, group_recv_sem,
    face_send_sem, face_recv_sem, edge_send_sem, edge_recv_sem, load_sem,
    up_sem, others_sem,
):
    g = lax.axis_index("grp")
    d = lax.axis_index("dev")
    obs_rows = resid.shape[0]
    per_dest = capacity // LANES
    half_dev = dev_count // 2
    row_total = half_dev * per_dest
    batch = dev_count // BATCHES
    per_block = 8 // per_dest

    def when(condition, action):
        @pl.when(condition)
        def _():
            action()

    def wrapped(step_g, step_d):
        return (
            lax.rem(g + step_g + grp_count, grp_count),
            lax.rem(d + step_d + dev_count, dev_count),
        )

    loads = [
        pltpu.make_async_copy(source, sink, load_sem.at[i])
        for i, (source, sink) in enumerate(
            zip(
                (dest_in, slot_in, resid_in, weight_in, coord_in, elem_in),
                (dest, slot, resid, weight, coord, elem),
            )
        )
    ]
    for load in loads:
        load.start()

    barrier = pltpu.get_barrier_semaphore()
    others = [wrapped(j, 0) for j in range(1, grp_count)]
    others += [wrapped(i, j) for i in (-1, 1) for j in (-1, 1)]

    def signal(semaphore, partner):
        pl.semaphore_signal(semaphore, inc=1, device_id=partner, device_id_type=MESH)

    def is_lower(partner):
        return (partner[1] < d) | ((partner[1] == d) & (partner[0] < g))

    for p in range(dev_count):
        when(p > d, lambda: signal(barrier, (g, p)))
    lower_count = d
    higher_others = len(others)
    for partner in others:
        lower = is_lower(partner)
        when(jnp.logical_not(lower), lambda: signal(barrier, partner))
        lower_count = lower_count + lower.astype(jnp.int32)
        higher_others = higher_others - lower.astype(jnp.int32)
    when(lower_count > 0, lambda: pl.semaphore_wait(barrier, lower_count))
    for p in range(dev_count):
        when(p < d, lambda: signal(up_sem.at[d], (g, p)))
    for partner in others:
        when(is_lower(partner), lambda: signal(others_sem, partner))

    for load in loads:
        load.wait()

    residual = resid[...]
    forcing = weight[...] * residual
    high, low = split2(forcing)
    where = dest[...]
    which = slot[...]
    terms[0] = ((where % half_dev) * per_dest + which // LANES).astype(F32)
    terms[1] = ((where // half_dev) * LANES + which % LANES).astype(F32)
    terms[2] = high
    terms[3] = low
    terms[4] = elem[...].astype(F32)
    part = jnp.sum(forcing * residual, axis=0, keepdims=True)
    cost_send[...] = jnp.broadcast_to(0.5 * jnp.sum(part, axis=1, keepdims=True), (1, LANES))

    row_ids = sublane_ids(row_total)
    lane_ids = sublane_ids(2 * LANES)
    for r in range(obs_rows):
        columns = slice(r * LANES, (r + 1) * LANES)
        row_hot = one_hot(terms[0, r : r + 1, :], row_ids)
        lane_hot[:, columns] = one_hot(terms[1, r : r + 1, :], lane_ids)
        coord_high, coord_low = split2(coord[:, columns])
        values = [coord_high[c : c + 1] for c in range(3)] + [terms[2, r : r + 1, :]]
        values += [terms[4, r : r + 1, :]]
        values += [coord_low[c : c + 1] for c in range(3)] + [terms[3, r : r + 1, :]]
        for i, value in enumerate(values):
            tile = jnp.broadcast_to(value, (row_total, LANES)).astype(BF16)
            left[i * row_total : (i + 1) * row_total, columns] = row_hot * tile
    packed = dot_nt(left[...], lane_hot[...])
    for p in range(dev_count):
        lanes = slice(p // half_dev * LANES, (p // half_dev + 1) * LANES)
        for c in range(5):
            start = c * row_total + p % half_dev * per_dest
            rows = packed[start : start + per_dest, lanes]
            if c < 4:
                start = (c + 5) * row_total + p % half_dev * per_dest
                rows = rows + packed[start : start + per_dest, lanes]
            send[p, c * per_dest : (c + 1) * per_dest, :] = rows

    def data_copy(p, source):
        return pltpu.make_async_remote_copy(
            src_ref=send.at[p], dst_ref=recv.at[source],
            send_sem=send_sem.at[p], recv_sem=recv_sem.at[source],
            device_id=(g, p), device_id_type=MESH,
        )

    def cost_copy(p, source):
        return pltpu.make_async_remote_copy(
            src_ref=cost_send, dst_ref=cost_recv.at[source],
            send_sem=cost_send_sem.at[p], recv_sem=cost_recv_sem.at[source],
            device_id=(g, p), device_id_type=MESH,
        )

    def group_copy(j):
        return pltpu.make_async_remote_copy(
            src_ref=group_send, dst_ref=group_recv.at[j],
            send_sem=group_send_sem.at[j], recv_sem=group_recv_sem.at[j],
            device_id=wrapped(j, 0), device_id_type=MESH,
        )

    own = d // batch

    def send_to(p):
        when(p > d, lambda: pl.semaphore_wait(up_sem.at[p], 1))
        data_copy(p, d).start()
        cost_copy(p, d).start()

    late = dev_count - batch
    for p in range(late):
        when(p != d, lambda: send_to(p))
    for p in range(late, dev_count):
        when((own == BATCHES - 1) & (p != d), lambda: send_to(p))
    recv[d] = send[d]

    def channels(x, j):
        def channel(c):
            rows = [
                recv[x * batch + j * per_block + i, c * per_dest : (c + 1) * per_dest, :]
                for i in range(per_block)
            ]
            return rows[0] if per_block == 1 else jnp.concatenate(rows, axis=0)

        return [channel(c) for c in range(5)]

    elem_ids = sublane_ids(ELEM_DEV)
    blocks = batch * capacity // CHUNK

    def prepare(x):
        for j in range(blocks):
            u, v, w, forcing, owner = channels(x, j)
            rows = slice(j * 8, j * 8 + 8)
            second_w = basis_values(v)
            weighted = [first * forcing for first in basis_values(u)]
            for c, value in enumerate(basis_values(w)):
                third[c, rows] = value
            for i, (a, b) in enumerate(PAIRS):
                outer[i, rows] = weighted[a] * second_w[b]
            for h in range(8):
                columns = slice((j * 8 + h) * LANES, (j * 8 + h + 1) * LANES)
                onehot[:, columns] = one_hot(owner[h : h + 1, :], elem_ids)

    face_count, inner_count = len(OUTER_PAIRS), len(INNER_PAIRS)

    def products(pairs, start):
        count = pairs.stop - pairs.start
        for h in range(blocks * 8):
            columns = slice(h * LANES, (h + 1) * LANES)
            value = outer[pairs, h : h + 1, :] * third[:, h, :][None]
            value = value.reshape(count * 8, LANES)
            rounded = value.astype(BF16)
            product[start : start + count * 8, columns] = rounded
            rest = (value - rounded.astype(F32)).astype(BF16)
            product[start + count * 8 : start + count * 16, columns] = rest

    def face_products():
        products(slice(0, face_count), 0)

    def inner_products():
        products(slice(face_count, len(PAIRS)), face_count * 16)

    def add_rows(sums, total, first):
        count = sums.shape[0]
        value = total[0:count] + total[count : 2 * count]
        if first:
            sums[...] = value
        else:
            sums[...] += value

    def all_rows(x, first):
        prepare(x)
        face_products()
        inner_products()
        total = dot_nt(product[...], onehot[...])
        add_rows(face_rows, total[0 : face_count * 16], first)
        add_rows(inner_rows, total[face_count * 16 :], first)

    def arrive(source):
        data_copy(source, source).wait_recv()

    for i in range(batch):
        when(own * batch + i != d, lambda: arrive(own * batch + i))
    all_rows(own, True)

    for p in range(late, dev_count):
        when(own != BATCHES - 1, lambda: send_to(p))

    def from_batch(t):
        x = t - 1 + (t > own).astype(jnp.int32)
        for i in range(batch):
            arrive(x * batch + i)
        return x

    def middle(t, carry):
        all_rows(from_batch(t), False)
        return carry

    lax.fori_loop(1, BATCHES - 1, middle, 0)
    prepare(from_batch(BATCHES - 1))
    face_products()
    total = dot_nt(product[0 : face_count * 16], onehot[...])
    add_rows(face_rows, total, False)

    def place(sums, pairs):
        for i, (a, b) in enumerate(pairs):
            start = a * 64 + b * 8
            raw[start : start + 8, :] = sums[i * 8 : i * 8 + 8, :]

    place(face_rows, OUTER_PAIRS)

    lane = lax.broadcasted_iota(jnp.int32, (1, LANES), 1)
    lower_half = lane < 64
    node = (lane // 8) % 8
    block = raw[448:512, 128:256]
    a_send[0] = jnp.where(lower_half, pltpu.roll(block[0:32], 64, 1), block[32:64])
    block = raw[0:64, 0:128]
    a_send[1] = jnp.where(lower_half, block[0:32], pltpu.roll(block[32:64], 64, 1))
    for half in range(2):
        columns = slice(half * LANES, (half + 1) * LANES)
        up = pltpu.roll(raw[56:64, columns], 72, 1)
        down = raw[0:8, columns]
        for a in range(1, 8):
            high = raw[a * 64 + 56 : a * 64 + 64, columns]
            low = raw[a * 64 : a * 64 + 8, columns]
            up = jnp.where(node == a, pltpu.roll(high, (a * 8 + 72) % 128, 1), up)
            down = jnp.where(node == a, pltpu.roll(low, a * 8, 1), down)
        b_send[0, half] = up
        b_send[1, half] = down

    steps = (1, -1)

    def face_copy(i):
        if i < 2:
            source, sink, target = a_send.at[i], a_recv.at[i], wrapped(steps[i], 0)
        else:
            source, sink, target = b_send.at[i - 2], b_recv.at[i - 2], wrapped(0, steps[i - 2])
        return pltpu.make_async_remote_copy(
            src_ref=source, dst_ref=sink,
            send_sem=face_send_sem.at[i], recv_sem=face_recv_sem.at[i],
            device_id=target, device_id_type=MESH,
        )

    def edge_copy(i, j):
        return pltpu.make_async_remote_copy(
            src_ref=b_send.at[j, 1 - i], dst_ref=edge_recv.at[j, i],
            send_sem=edge_send_sem.at[j, i], recv_sem=edge_recv_sem.at[j, i],
            device_id=wrapped(steps[i], steps[j]), device_id_type=MESH,
        )

    sends_a, sends_b = (g < grp_count - 1, g > 0), (d < dev_count - 1, d > 0)
    gets_a, gets_b = (g > 0, g < grp_count - 1), (d > 0, d < dev_count - 1)

    def clear(ref, i):
        ref[i] = jnp.zeros_like(ref[i])

    when(higher_others > 0, lambda: pl.semaphore_wait(others_sem, higher_others))
    for j in range(2):
        for i in range(2):
            when(sends_a[i] & sends_b[j], lambda: edge_copy(i, j).start())
    for i in range(2):
        when(sends_a[i], lambda: face_copy(i).start())
        when(sends_b[i], lambda: face_copy(2 + i).start())

    group_cost = cost_send[...]
    for i in range(dev_count):
        when(i != d, lambda: cost_copy(i, i).wait_recv())
        group_cost = group_cost + jnp.where(i == d, 0.0, cost_recv[i])
    group_send[...] = group_cost
    for j in range(1, grp_count):
        group_copy(j).start()

    inner_products()
    total = dot_nt(product[face_count * 16 :], onehot[...])
    add_rows(inner_rows, total, False)
    place(inner_rows, INNER_PAIRS)

    for i in range(2):
        when(gets_a[i], lambda: face_copy(i).wait_recv())
        when(jnp.logical_not(gets_a[i]), lambda: clear(a_recv, i))
    low, high = raw[0:64, :], raw[448:512, :]
    from_low, from_high = a_recv[0], a_recv[1]
    from_low = jnp.concatenate([from_low, pltpu.roll(from_low, 64, 1)], axis=0)
    from_high = jnp.concatenate([pltpu.roll(from_high, 64, 1), from_high], axis=0)
    high_rolled = [pltpu.roll(high[:, :128], 64, 1), pltpu.roll(high[:, 128:], 64, 1)]
    low_rolled = [pltpu.roll(low[:, :128], 64, 1), pltpu.roll(low[:, 128:], 64, 1)]
    raw[0:64, 0:128] = low[:, :128] + jnp.where(lower_half, from_low, high_rolled[0])
    raw[0:64, 128:256] = low[:, 128:] + jnp.where(lower_half, high_rolled[0], high_rolled[1])
    raw[448:512, 0:128] = high[:, :128] + jnp.where(lower_half, low_rolled[0], low_rolled[1])
    raw[448:512, 128:256] = high[:, 128:] + jnp.where(lower_half, low_rolled[1], from_high)

    faces = []
    for j in range(2):
        when(gets_b[j], lambda: face_copy(2 + j).wait_recv())
        when(jnp.logical_not(gets_b[j]), lambda: clear(b_recv, j))
        for i in range(2):
            both = gets_a[i] & gets_b[j]
            when(both, lambda: edge_copy(i, j).wait_recv())
            when(jnp.logical_not(both), lambda: clear(edge_recv, (j, i)))
        first, second = b_recv[j, 0], b_recv[j, 1]
        up = [pltpu.roll(x, 8, 1) for x in (edge_recv[j, 0], first, second)]
        down = [pltpu.roll(x, 120, 1) for x in (first, second, edge_recv[j, 1])]
        face = []
        for half, own in enumerate((first, second)):
            from_low = jnp.where(lower_half, up[half], up[half + 1])
            from_high = jnp.where(lower_half, down[half], down[half + 1])
            face.append(
                own + jnp.where(node == 0, from_low, jnp.where(node == 7, from_high, 0.0))
            )
        faces.append(face)
    for half in range(2):
        columns = slice(half * LANES, (half + 1) * LANES)
        for a in range(8):
            low_rows = slice(a * 64, a * 64 + 8)
            high_rows = slice(a * 64 + 56, a * 64 + 64)
            low, high = raw[low_rows, columns], raw[high_rows, columns]
            got_low = pltpu.roll(faces[0][half], (128 - a * 8) % 128, 1)
            got_high = pltpu.roll(faces[1][half], (56 - a * 8) % 128, 1)
            raw[low_rows, columns] = low + jnp.where(node == 0, got_low, pltpu.roll(high, 8, 1))
            raw[high_rows, columns] = high + jnp.where(node == 7, got_high, pltpu.roll(low, 120, 1))

    ez = lax.broadcasted_iota(jnp.int32, (1, 8, LANES), 2) % 8
    c = lax.broadcasted_iota(jnp.int32, (1, 8, LANES), 1)
    takes_low = (c == 0) & (ez > 0)
    takes_high = (c == 7) & (ez < 7)
    for half in range(2):
        for part in range(4):
            rows = slice(part * 128, (part + 1) * 128)
            field = raw[rows, half * LANES : (half + 1) * LANES].reshape(16, 8, LANES)
            below = pltpu.roll(pltpu.roll(field, 1, 2), 1, 1)
            above = pltpu.roll(pltpu.roll(field, 127, 2), 7, 1)
            field = field + jnp.where(takes_low, below, jnp.where(takes_high, above, 0.0))
            out[half * LANES : (half + 1) * LANES, rows] = field.reshape(128, LANES).T

    all_cost = group_send[...]
    for j in range(1, grp_count):
        group_copy(j).wait_recv()
        all_cost = all_cost + group_recv[j]
    cost[...] = all_cost

    for p in range(dev_count):
        when(p != d, lambda: data_copy(p, p).wait_send())
        when(p != d, lambda: cost_copy(p, p).wait_send())
    for j in range(1, grp_count):
        group_copy(j).wait_send()
    for i in range(2):
        when(sends_a[i], lambda: face_copy(i).wait_send())
        when(sends_b[i], lambda: face_copy(2 + i).wait_send())
        for j in range(2):
            when(sends_a[i] & sends_b[j], lambda: edge_copy(i, j).wait_send())


def on_device(obs_coord, obs_resid, obs_weight, obs_dest, obs_send_slot, obs_elem, obs_slot):
    dev_count = lax.axis_size("dev")
    grp_count = lax.axis_size("grp")
    row_count = obs_resid.shape[0]
    obs_rows = row_count // LANES
    capacity = 2 * row_count // dev_count
    per_dest = capacity // LANES
    packed_rows = dev_count // 2 * per_dest
    batch_obs = dev_count // BATCHES * capacity
    vmem = pl.BlockSpec(memory_space=pltpu.VMEM)
    dma = pltpu.SemaphoreType.DMA
    regular = pltpu.SemaphoreType.REGULAR
    rows = [
        x.reshape(obs_rows, LANES)
        for x in (obs_resid, obs_weight, obs_dest, obs_send_slot, obs_elem)
    ]
    field, cost = pl.pallas_call(
        functools.partial(kernel, dev_count, grp_count, capacity),
        out_shape=(
            pltpu.VMEM((ELEM_DEV, 512), F32),
            pltpu.VMEM((1, LANES), F32),
        ),
        in_specs=[pl.BlockSpec(memory_space=pl.ANY)] * 6,
        out_specs=(vmem, vmem),
        scratch_shapes=[
            pltpu.VMEM((3, row_count), F32),
            pltpu.VMEM((obs_rows, LANES), F32),
            pltpu.VMEM((obs_rows, LANES), F32),
            pltpu.VMEM((obs_rows, LANES), jnp.int32),
            pltpu.VMEM((obs_rows, LANES), jnp.int32),
            pltpu.VMEM((obs_rows, LANES), jnp.int32),
            pltpu.VMEM((5, obs_rows, LANES), F32),
            pltpu.VMEM((9 * packed_rows, row_count), BF16),
            pltpu.VMEM((2 * LANES, row_count), BF16),
            pltpu.VMEM((dev_count, 5 * per_dest, LANES), F32),
            pltpu.VMEM((dev_count, 5 * per_dest, LANES), F32),
            pltpu.VMEM((1, LANES), F32),
            pltpu.VMEM((dev_count, 1, LANES), F32),
            pltpu.VMEM((1, LANES), F32),
            pltpu.VMEM((grp_count, 1, LANES), F32),
            pltpu.VMEM((8, batch_obs // LANES, LANES), F32),
            pltpu.VMEM((64, batch_obs // LANES, LANES), F32),
            pltpu.VMEM((1024, batch_obs), BF16),
            pltpu.VMEM((ELEM_DEV, batch_obs), BF16),
            pltpu.VMEM((512, ELEM_DEV), F32),
            pltpu.VMEM((2, 32, LANES), F32),
            pltpu.VMEM((2, 32, LANES), F32),
            pltpu.VMEM((2, 2, 8, LANES), F32),
            pltpu.VMEM((2, 2, 8, LANES), F32),
            pltpu.VMEM((2, 2, 8, LANES), F32),
            pltpu.VMEM((len(OUTER_PAIRS) * 8, ELEM_DEV), F32),
            pltpu.VMEM((len(INNER_PAIRS) * 8, ELEM_DEV), F32),
            dma((dev_count,)),
            dma((dev_count,)),
            dma((dev_count,)),
            dma((dev_count,)),
            dma((grp_count,)),
            dma((grp_count,)),
            dma((4,)),
            dma((4,)),
            dma((2, 2)),
            dma((2, 2)),
            dma((6,)),
            regular((dev_count,)),
            regular,
        ],
        compiler_params=pltpu.CompilerParams(collective_id=0, has_side_effects=True),
    )(obs_coord, *rows)
    return field.reshape(EX, EY, EZ, 512), cost[0, 0]


def solution(mesh):
    placed = (
        P(None, ("grp", "dev")),
        P(("grp", "dev")),
        P(("grp", "dev")),
        P(("grp", "dev")),
        P(("grp", "dev")),
        P(("grp", "dev")),
        P(("grp", "dev")),
    )
    return jax.shard_map(
        on_device,
        mesh=mesh,
        in_specs=placed,
        out_specs=(P("grp", "dev", None, None), P()),
        check_vma=False,
    )
```

```python
import functools
import math

import jax
import jax.numpy as jnp
from jax import lax
from jax.experimental import pallas as pl
from jax.experimental.pallas import tpu as pltpu
from jax.sharding import PartitionSpec as P

EX = 4
EY = 8
EZ = 8
ELEM_DEV = 256
LANES = 128
SLOTS = 32
CHANNELS = 6
BATCHES = 4
MESH = pl.DeviceIdType.MESH
F32 = jnp.float32
BF16 = jnp.bfloat16

ANCHORS = [-math.cos(math.pi * k / 7) for k in range(8)]
OUTER_PAIRS = [(a, b) for a in (0, 7) for b in range(8)]
OUTER_PAIRS += [(a, b) for a in range(1, 7) for b in (0, 7)]
INNER_PAIRS = [(a, b) for a in range(1, 7) for b in range(1, 7)]
PAIRS = OUTER_PAIRS + INNER_PAIRS
COEFS = [
    1.0 / math.prod(ANCHORS[a] - ANCHORS[m] for m in range(8) if m != a) for a in range(8)
]


def basis_values(t):
    factors = [t - p for p in ANCHORS]
    prefix = [None] * 8
    suffix = [None] * 8
    for k in range(1, 8):
        prefix[k] = factors[k - 1] if k == 1 else prefix[k - 1] * factors[k - 1]
    for k in range(6, -1, -1):
        suffix[k] = factors[k + 1] if k == 6 else suffix[k + 1] * factors[k + 1]
    basis = []
    for a in range(8):
        if a == 0:
            product = suffix[0]
        elif a == 7:
            product = prefix[7]
        else:
            product = prefix[a] * suffix[a]
        basis.append(product * COEFS[a])
    return basis


def dot_nt(left, right):
    return lax.dot_general(left, right, (((1,), (1,)), ((), ())), preferred_element_type=F32)


def halves(row):
    value = jnp.broadcast_to(row, (16, LANES))
    first = value.astype(BF16)
    return first, (value - first.astype(F32)).astype(BF16)


def one_hot(row, ids):
    tile = jnp.broadcast_to(row, (16, LANES)).astype(BF16)
    return [jnp.where(part == tile, jnp.ones((), BF16), jnp.zeros((), BF16)) for part in ids]


def spread(hot, tiles):
    return jnp.concatenate([part * tile for tile in tiles for part in hot], axis=0)


def sublane_ids(count):
    ids = lax.broadcasted_iota(jnp.int32, (16, LANES), 0)
    return [(ids + 16 * i).astype(F32).astype(BF16) for i in range(count // 16)]


def kernel(
    dev_count, grp_count, capacity,
    coord_in, resid_in, weight_in, dest_in, send_slot_in, elem_in, slot_in,
    out, cost,
    coord, resid, weight, dest, send_slot, elem, slot, terms, send, recv,
    cost_send, cost_recv, group_send, group_recv,
    grid, first, second, third, raw, a_send, a_recv, b_send, b_recv, edge_recv,
    send_sem, recv_sem, cost_send_sem, cost_recv_sem, group_send_sem, group_recv_sem,
    face_send_sem, face_recv_sem, edge_send_sem, edge_recv_sem, load_sem,
    up_sem, others_sem,
):
    g = lax.axis_index("grp")
    d = lax.axis_index("dev")
    obs_rows = resid.shape[0]
    per_dest = capacity // LANES
    half_dev = dev_count // 2
    row_total = half_dev * per_dest
    batch = dev_count // BATCHES

    def when(condition, action):
        @pl.when(condition)
        def _():
            action()

    def wrapped(step_g, step_d):
        return (
            lax.rem(g + step_g + grp_count, grp_count),
            lax.rem(d + step_d + dev_count, dev_count),
        )

    loads = [
        pltpu.make_async_copy(source, sink, load_sem.at[i])
        for i, (source, sink) in enumerate(
            zip(
                (dest_in, send_slot_in, resid_in, weight_in, coord_in, elem_in, slot_in),
                (dest, send_slot, resid, weight, coord, elem, slot),
            )
        )
    ]
    for load in loads:
        load.start()

    barrier = pltpu.get_barrier_semaphore()
    others = [wrapped(j, 0) for j in range(1, grp_count)]
    others += [wrapped(i, j) for i in (-1, 1) for j in (-1, 1)]

    def signal(semaphore, partner):
        pl.semaphore_signal(semaphore, inc=1, device_id=partner, device_id_type=MESH)

    def is_lower(partner):
        return (partner[1] < d) | ((partner[1] == d) & (partner[0] < g))

    for p in range(dev_count):
        when(p > d, lambda: signal(barrier, (g, p)))
    lower_count = d
    higher_others = len(others)
    for partner in others:
        lower = is_lower(partner)
        when(jnp.logical_not(lower), lambda: signal(barrier, partner))
        lower_count = lower_count + lower.astype(jnp.int32)
        higher_others = higher_others - lower.astype(jnp.int32)
    when(lower_count > 0, lambda: pl.semaphore_wait(barrier, lower_count))
    for p in range(dev_count):
        when(p < d, lambda: signal(up_sem.at[d], (g, p)))
    for partner in others:
        when(is_lower(partner), lambda: signal(others_sem, partner))

    for load in loads:
        load.wait()

    residual = resid[...]
    forcing = weight[...] * residual
    where = dest[...]
    which = send_slot[...]
    terms[0] = ((where % half_dev) * per_dest + which // LANES).astype(F32)
    terms[1] = ((where // half_dev) * LANES + which % LANES).astype(F32)
    terms[2] = forcing
    terms[3] = elem[...].astype(F32)
    terms[4] = slot[...].astype(F32)
    part = jnp.sum(forcing * residual, axis=0, keepdims=True)
    cost_send[...] = jnp.broadcast_to(0.5 * jnp.sum(part, axis=1, keepdims=True), (1, LANES))

    row_ids = sublane_ids(row_total)
    lane_ids = sublane_ids(2 * LANES)
    left, right = [], []
    for r in range(obs_rows):
        columns = slice(r * LANES, (r + 1) * LANES)
        values = [halves(coord[c : c + 1, columns]) for c in range(3)]
        values.append(halves(terms[2, r : r + 1, :]))
        tiles = [high for high, _ in values]
        tiles += [halves(terms[i, r : r + 1, :])[0] for i in (3, 4)]
        tiles += [low for _, low in values]
        left.append(spread(one_hot(terms[0, r : r + 1, :], row_ids), tiles))
        right.append(jnp.concatenate(one_hot(terms[1, r : r + 1, :], lane_ids), axis=0))
    packed = dot_nt(jnp.concatenate(left, axis=1), jnp.concatenate(right, axis=1))
    for p in range(dev_count):
        lanes = slice(p // half_dev * LANES, (p // half_dev + 1) * LANES)
        for c in range(CHANNELS):
            start = c * row_total + p % half_dev * per_dest
            rows = packed[start : start + per_dest, lanes]
            if c < 4:
                start = (c + CHANNELS) * row_total + p % half_dev * per_dest
                rows = rows + packed[start : start + per_dest, lanes]
            send[p, c * per_dest : (c + 1) * per_dest, :] = rows

    def data_copy(p, source):
        return pltpu.make_async_remote_copy(
            src_ref=send.at[p], dst_ref=recv.at[source],
            send_sem=send_sem.at[p], recv_sem=recv_sem.at[source],
            device_id=(g, p), device_id_type=MESH,
        )

    def cost_copy(p, source):
        return pltpu.make_async_remote_copy(
            src_ref=cost_send, dst_ref=cost_recv.at[source],
            send_sem=cost_send_sem.at[p], recv_sem=cost_recv_sem.at[source],
            device_id=(g, p), device_id_type=MESH,
        )

    def group_copy(j):
        return pltpu.make_async_remote_copy(
            src_ref=group_send, dst_ref=group_recv.at[j],
            send_sem=group_send_sem.at[j], recv_sem=group_recv_sem.at[j],
            device_id=wrapped(j, 0), device_id_type=MESH,
        )

    own = d // batch

    def send_to(p):
        when(p > d, lambda: pl.semaphore_wait(up_sem.at[p], 1))
        data_copy(p, d).start()
        cost_copy(p, d).start()

    for p in range(dev_count):
        when(p != d, lambda: send_to(p))
    recv[d] = send[d]

    elem_ids = sublane_ids(ELEM_DEV)
    slot_ids = sublane_ids(SLOTS)

    def scatter(x, fresh):
        left, right = [], []
        for r in range(batch * per_dest):
            source = x * batch + r // per_dest

            def row(c):
                start = c * per_dest + r % per_dest
                return recv[source, start : start + 1, :]

            values = [halves(row(c)) for c in range(4)]
            tiles = [high for high, _ in values] + [low for _, low in values]
            left.append(spread(one_hot(row(5), slot_ids), tiles))
            right.append(jnp.concatenate(one_hot(row(4), elem_ids), axis=0))
        total = dot_nt(jnp.concatenate(left, axis=1), jnp.concatenate(right, axis=1))
        if fresh:
            grid[...] = total
        else:
            grid[...] += total

    def arrive(source):
        data_copy(source, source).wait_recv()

    for i in range(batch):
        when(own * batch + i != d, lambda: arrive(own * batch + i))
    scatter(own, True)

    def from_batch(t, carry):
        x = t - 1 + (t > own).astype(jnp.int32)
        for i in range(batch):
            arrive(x * batch + i)
        scatter(x, False)
        return carry

    lax.fori_loop(1, BATCHES, from_batch, 0)

    for half in range(2):
        lanes = slice(half * LANES, (half + 1) * LANES)

        def field(c):
            high = grid[c * SLOTS : (c + 1) * SLOTS, lanes]
            return high + grid[(c + 4) * SLOTS : (c + 5) * SLOTS, lanes]

        forcing = field(3)
        for values, sink in zip(range(3), (first, second, third)):
            for k, value in enumerate(basis_values(field(values))):
                value = value * forcing if values == 0 else value
                sink[half, k * SLOTS : (k + 1) * SLOTS, :] = value

    def contract(pairs):
        for half in range(2):
            sums = [None] * len(pairs)
            for s in range(SLOTS):
                w = third[half, pl.ds(s, 8, stride=SLOTS), :]
                u, vw = {}, {}
                for a, b in pairs:
                    if a not in u:
                        row = first[half, a * SLOTS + s : a * SLOTS + s + 1, :]
                        u[a] = jnp.broadcast_to(row, (8, LANES))
                    if b not in vw:
                        vw[b] = second[half, b * SLOTS + s : b * SLOTS + s + 1, :] * w
                for i, (a, b) in enumerate(pairs):
                    value = u[a] * vw[b]
                    sums[i] = value if sums[i] is None else sums[i] + value
            for (a, b), value in zip(pairs, sums):
                start = a * 64 + b * 8
                raw[start : start + 8, half * LANES : (half + 1) * LANES] = value

    contract(OUTER_PAIRS)

    lane = lax.broadcasted_iota(jnp.int32, (1, LANES), 1)
    lower_half = lane < 64
    node = (lane // 8) % 8
    block = raw[448:512, 128:256]
    a_send[0] = jnp.where(lower_half, pltpu.roll(block[0:32], 64, 1), block[32:64])
    block = raw[0:64, 0:128]
    a_send[1] = jnp.where(lower_half, block[0:32], pltpu.roll(block[32:64], 64, 1))
    for half in range(2):
        columns = slice(half * LANES, (half + 1) * LANES)
        up = pltpu.roll(raw[56:64, columns], 72, 1)
        down = raw[0:8, columns]
        for a in range(1, 8):
            high = raw[a * 64 + 56 : a * 64 + 64, columns]
            low = raw[a * 64 : a * 64 + 8, columns]
            up = jnp.where(node == a, pltpu.roll(high, (a * 8 + 72) % 128, 1), up)
            down = jnp.where(node == a, pltpu.roll(low, a * 8, 1), down)
        b_send[0, half] = up
        b_send[1, half] = down

    steps = (1, -1)

    def face_copy(i):
        if i < 2:
            source, sink, target = a_send.at[i], a_recv.at[i], wrapped(steps[i], 0)
        else:
            source, sink, target = b_send.at[i - 2], b_recv.at[i - 2], wrapped(0, steps[i - 2])
        return pltpu.make_async_remote_copy(
            src_ref=source, dst_ref=sink,
            send_sem=face_send_sem.at[i], recv_sem=face_recv_sem.at[i],
            device_id=target, device_id_type=MESH,
        )

    def edge_copy(i, j):
        return pltpu.make_async_remote_copy(
            src_ref=b_send.at[j, 1 - i], dst_ref=edge_recv.at[j, i],
            send_sem=edge_send_sem.at[j, i], recv_sem=edge_recv_sem.at[j, i],
            device_id=wrapped(steps[i], steps[j]), device_id_type=MESH,
        )

    sends_a, sends_b = (g < grp_count - 1, g > 0), (d < dev_count - 1, d > 0)
    gets_a, gets_b = (g > 0, g < grp_count - 1), (d > 0, d < dev_count - 1)

    def clear(ref, i):
        ref[i] = jnp.zeros_like(ref[i])

    when(higher_others > 0, lambda: pl.semaphore_wait(others_sem, higher_others))
    for j in range(2):
        for i in range(2):
            when(sends_a[i] & sends_b[j], lambda: edge_copy(i, j).start())
    for i in range(2):
        when(sends_a[i], lambda: face_copy(i).start())
        when(sends_b[i], lambda: face_copy(2 + i).start())

    group_cost = cost_send[...]
    for i in range(dev_count):
        when(i != d, lambda: cost_copy(i, i).wait_recv())
        group_cost = group_cost + jnp.where(i == d, 0.0, cost_recv[i])
    group_send[...] = group_cost
    for j in range(1, grp_count):
        group_copy(j).start()

    contract([pair for pair in INNER_PAIRS if pair[1] < 4])
    contract([pair for pair in INNER_PAIRS if pair[1] >= 4])

    for i in range(2):
        when(gets_a[i], lambda: face_copy(i).wait_recv())
        when(jnp.logical_not(gets_a[i]), lambda: clear(a_recv, i))
    low, high = raw[0:64, :], raw[448:512, :]
    from_low, from_high = a_recv[0], a_recv[1]
    from_low = jnp.concatenate([from_low, pltpu.roll(from_low, 64, 1)], axis=0)
    from_high = jnp.concatenate([pltpu.roll(from_high, 64, 1), from_high], axis=0)
    high_rolled = [pltpu.roll(high[:, :128], 64, 1), pltpu.roll(high[:, 128:], 64, 1)]
    low_rolled = [pltpu.roll(low[:, :128], 64, 1), pltpu.roll(low[:, 128:], 64, 1)]
    raw[0:64, 0:128] = low[:, :128] + jnp.where(lower_half, from_low, high_rolled[0])
    raw[0:64, 128:256] = low[:, 128:] + jnp.where(lower_half, high_rolled[0], high_rolled[1])
    raw[448:512, 0:128] = high[:, :128] + jnp.where(lower_half, low_rolled[0], low_rolled[1])
    raw[448:512, 128:256] = high[:, 128:] + jnp.where(lower_half, low_rolled[1], from_high)

    faces = []
    for j in range(2):
        when(gets_b[j], lambda: face_copy(2 + j).wait_recv())
        when(jnp.logical_not(gets_b[j]), lambda: clear(b_recv, j))
        for i in range(2):
            both = gets_a[i] & gets_b[j]
            when(both, lambda: edge_copy(i, j).wait_recv())
            when(jnp.logical_not(both), lambda: clear(edge_recv, (j, i)))
        first, second = b_recv[j, 0], b_recv[j, 1]
        up = [pltpu.roll(x, 8, 1) for x in (edge_recv[j, 0], first, second)]
        down = [pltpu.roll(x, 120, 1) for x in (first, second, edge_recv[j, 1])]
        face = []
        for half, own in enumerate((first, second)):
            from_low = jnp.where(lower_half, up[half], up[half + 1])
            from_high = jnp.where(lower_half, down[half], down[half + 1])
            face.append(
                own + jnp.where(node == 0, from_low, jnp.where(node == 7, from_high, 0.0))
            )
        faces.append(face)
    for half in range(2):
        columns = slice(half * LANES, (half + 1) * LANES)
        for a in range(8):
            low_rows = slice(a * 64, a * 64 + 8)
            high_rows = slice(a * 64 + 56, a * 64 + 64)
            low, high = raw[low_rows, columns], raw[high_rows, columns]
            got_low = pltpu.roll(faces[0][half], (128 - a * 8) % 128, 1)
            got_high = pltpu.roll(faces[1][half], (56 - a * 8) % 128, 1)
            raw[low_rows, columns] = low + jnp.where(node == 0, got_low, pltpu.roll(high, 8, 1))
            raw[high_rows, columns] = high + jnp.where(node == 7, got_high, pltpu.roll(low, 120, 1))

    ez = lax.broadcasted_iota(jnp.int32, (1, 8, LANES), 2) % 8
    c = lax.broadcasted_iota(jnp.int32, (1, 8, LANES), 1)
    takes_low = (c == 0) & (ez > 0)
    takes_high = (c == 7) & (ez < 7)
    for half in range(2):
        for part in range(4):
            rows = slice(part * 128, (part + 1) * 128)
            field = raw[rows, half * LANES : (half + 1) * LANES].reshape(16, 8, LANES)
            below = pltpu.roll(pltpu.roll(field, 1, 2), 1, 1)
            above = pltpu.roll(pltpu.roll(field, 127, 2), 7, 1)
            field = field + jnp.where(takes_low, below, jnp.where(takes_high, above, 0.0))
            out[half * LANES : (half + 1) * LANES, rows] = field.reshape(128, LANES).T

    all_cost = group_send[...]
    for j in range(1, grp_count):
        group_copy(j).wait_recv()
        all_cost = all_cost + group_recv[j]
    cost[...] = all_cost

    for p in range(dev_count):
        when(p != d, lambda: data_copy(p, p).wait_send())
        when(p != d, lambda: cost_copy(p, p).wait_send())
    for j in range(1, grp_count):
        group_copy(j).wait_send()
    for i in range(2):
        when(sends_a[i], lambda: face_copy(i).wait_send())
        when(sends_b[i], lambda: face_copy(2 + i).wait_send())
        for j in range(2):
            when(sends_a[i] & sends_b[j], lambda: edge_copy(i, j).wait_send())


def on_device(obs_coord, obs_resid, obs_weight, obs_dest, obs_send_slot, obs_elem, obs_slot):
    dev_count = lax.axis_size("dev")
    grp_count = lax.axis_size("grp")
    row_count = obs_resid.shape[0]
    obs_rows = row_count // LANES
    capacity = 2 * row_count // dev_count
    per_dest = capacity // LANES
    vmem = pl.BlockSpec(memory_space=pltpu.VMEM)
    dma = pltpu.SemaphoreType.DMA
    regular = pltpu.SemaphoreType.REGULAR
    rows = [
        x.reshape(obs_rows, LANES)
        for x in (obs_resid, obs_weight, obs_dest, obs_send_slot, obs_elem, obs_slot)
    ]
    field, cost = pl.pallas_call(
        functools.partial(kernel, dev_count, grp_count, capacity),
        out_shape=(
            pltpu.VMEM((ELEM_DEV, 512), F32),
            pltpu.VMEM((1, LANES), F32),
        ),
        in_specs=[pl.BlockSpec(memory_space=pl.ANY)] * 7,
        out_specs=(vmem, vmem),
        scratch_shapes=[
            pltpu.VMEM((3, row_count), F32),
            pltpu.VMEM((obs_rows, LANES), F32),
            pltpu.VMEM((obs_rows, LANES), F32),
            pltpu.VMEM((obs_rows, LANES), jnp.int32),
            pltpu.VMEM((obs_rows, LANES), jnp.int32),
            pltpu.VMEM((obs_rows, LANES), jnp.int32),
            pltpu.VMEM((obs_rows, LANES), jnp.int32),
            pltpu.VMEM((5, obs_rows, LANES), F32),
            pltpu.VMEM((dev_count, CHANNELS * per_dest, LANES), F32),
            pltpu.VMEM((dev_count, CHANNELS * per_dest, LANES), F32),
            pltpu.VMEM((1, LANES), F32),
            pltpu.VMEM((dev_count, 1, LANES), F32),
            pltpu.VMEM((1, LANES), F32),
            pltpu.VMEM((grp_count, 1, LANES), F32),
            pltpu.VMEM((8 * SLOTS, ELEM_DEV), F32),
            pltpu.VMEM((2, 8 * SLOTS, LANES), F32),
            pltpu.VMEM((2, 8 * SLOTS, LANES), F32),
            pltpu.VMEM((2, 8 * SLOTS, LANES), F32),
            pltpu.VMEM((512, ELEM_DEV), F32),
            pltpu.VMEM((2, 32, LANES), F32),
            pltpu.VMEM((2, 32, LANES), F32),
            pltpu.VMEM((2, 2, 8, LANES), F32),
            pltpu.VMEM((2, 2, 8, LANES), F32),
            pltpu.VMEM((2, 2, 8, LANES), F32),
            dma((dev_count,)),
            dma((dev_count,)),
            dma((dev_count,)),
            dma((dev_count,)),
            dma((grp_count,)),
            dma((grp_count,)),
            dma((4,)),
            dma((4,)),
            dma((2, 2)),
            dma((2, 2)),
            dma((7,)),
            regular((dev_count,)),
            regular,
        ],
        compiler_params=pltpu.CompilerParams(collective_id=0, has_side_effects=True),
    )(obs_coord, *rows)
    return field.reshape(EX, EY, EZ, 512), cost[0, 0]


def solution(mesh):
    placed = (
        P(None, ("grp", "dev")),
        P(("grp", "dev")),
        P(("grp", "dev")),
        P(("grp", "dev")),
        P(("grp", "dev")),
        P(("grp", "dev")),
        P(("grp", "dev")),
    )
    return jax.shard_map(
        on_device,
        mesh=mesh,
        in_specs=placed,
        out_specs=(P("grp", "dev", None, None), P()),
        check_vma=False,
    )
```

```python
import functools
import math

import jax
import jax.numpy as jnp
from jax import lax
from jax.experimental import pallas as pl
from jax.experimental.pallas import tpu as pltpu
from jax.sharding import PartitionSpec as P

EX = 4
EY = 8
EZ = 8
ELEM_DEV = 256
LANES = 128
CHANNELS = 5
BATCHES = 4
MESH = pl.DeviceIdType.MESH
F32 = jnp.float32
BF16 = jnp.bfloat16

ANCHORS = [-math.cos(math.pi * k / 7) for k in range(8)]
OUTER_PAIRS = [(a, b) for a in (0, 7) for b in range(8)]
OUTER_PAIRS += [(a, b) for a in range(1, 7) for b in (0, 7)]
INNER_PAIRS = [(a, b) for a in range(1, 7) for b in range(1, 7)]
PAIRS = OUTER_PAIRS + INNER_PAIRS
COEFS = [
    1.0 / math.prod(ANCHORS[a] - ANCHORS[m] for m in range(8) if m != a) for a in range(8)
]


def basis_values(t):
    factors = [t - p for p in ANCHORS]
    prefix = [None] * 8
    suffix = [None] * 8
    for k in range(1, 8):
        prefix[k] = factors[k - 1] if k == 1 else prefix[k - 1] * factors[k - 1]
    for k in range(6, -1, -1):
        suffix[k] = factors[k + 1] if k == 6 else suffix[k + 1] * factors[k + 1]
    basis = []
    for a in range(8):
        if a == 0:
            product = suffix[0]
        elif a == 7:
            product = prefix[7]
        else:
            product = prefix[a] * suffix[a]
        basis.append(product * COEFS[a])
    return basis


def dot_nt(left, right):
    return lax.dot_general(left, right, (((1,), (1,)), ((), ())), preferred_element_type=F32)


def halves(row):
    value = jnp.broadcast_to(row, (16, LANES))
    first = value.astype(BF16)
    return first, (value - first.astype(F32)).astype(BF16)


def one_hot(row, ids):
    tile = jnp.broadcast_to(row, (16, LANES)).astype(BF16)
    return [jnp.where(part == tile, jnp.ones((), BF16), jnp.zeros((), BF16)) for part in ids]


def spread(hot, tiles):
    return jnp.concatenate([part * tile for tile in tiles for part in hot], axis=0)


def sublane_ids(count):
    ids = lax.broadcasted_iota(jnp.int32, (16, LANES), 0)
    return [(ids + 16 * i).astype(F32).astype(BF16) for i in range(count // 16)]


def kernel(
    dev_count, grp_count, capacity,
    coord_in, resid_in, weight_in, dest_in, slot_in, elem_in,
    out, cost,
    coord, resid, weight, dest, slot, elem, terms, send, recv,
    cost_send, cost_recv, group_send, group_recv,
    outer, third, face_rows, inner_rows, raw, a_send, a_recv, b_send, b_recv, edge_recv,
    send_sem, recv_sem, cost_send_sem, cost_recv_sem, group_send_sem, group_recv_sem,
    face_send_sem, face_recv_sem, edge_send_sem, edge_recv_sem, load_sem,
    up_sem, others_sem,
):
    g = lax.axis_index("grp")
    d = lax.axis_index("dev")
    obs_rows = resid.shape[0]
    per_dest = capacity // LANES
    half_dev = dev_count // 2
    row_total = half_dev * per_dest
    batch = dev_count // BATCHES

    def when(condition, action):
        @pl.when(condition)
        def _():
            action()

    def wrapped(step_g, step_d):
        return (
            lax.rem(g + step_g + grp_count, grp_count),
            lax.rem(d + step_d + dev_count, dev_count),
        )

    loads = [
        pltpu.make_async_copy(source, sink, load_sem.at[i])
        for i, (source, sink) in enumerate(
            zip(
                (dest_in, slot_in, resid_in, weight_in, coord_in, elem_in),
                (dest, slot, resid, weight, coord, elem),
            )
        )
    ]
    for load in loads:
        load.start()

    barrier = pltpu.get_barrier_semaphore()
    others = [wrapped(j, 0) for j in range(1, grp_count)]
    others += [wrapped(i, j) for i in (-1, 1) for j in (-1, 1)]

    def signal(semaphore, partner):
        pl.semaphore_signal(semaphore, inc=1, device_id=partner, device_id_type=MESH)

    def is_lower(partner):
        return (partner[1] < d) | ((partner[1] == d) & (partner[0] < g))

    for p in range(dev_count):
        when(p > d, lambda: signal(barrier, (g, p)))
    lower_count = d
    higher_others = len(others)
    for partner in others:
        lower = is_lower(partner)
        when(jnp.logical_not(lower), lambda: signal(barrier, partner))
        lower_count = lower_count + lower.astype(jnp.int32)
        higher_others = higher_others - lower.astype(jnp.int32)
    when(lower_count > 0, lambda: pl.semaphore_wait(barrier, lower_count))
    for p in range(dev_count):
        when(p < d, lambda: signal(up_sem.at[d], (g, p)))
    for partner in others:
        when(is_lower(partner), lambda: signal(others_sem, partner))

    for load in loads:
        load.wait()

    residual = resid[...]
    forcing = weight[...] * residual
    where = dest[...]
    which = slot[...]
    terms[0] = ((where % half_dev) * per_dest + which // LANES).astype(F32)
    terms[1] = ((where // half_dev) * LANES + which % LANES).astype(F32)
    terms[2] = forcing
    terms[3] = elem[...].astype(F32)
    part = jnp.sum(forcing * residual, axis=0, keepdims=True)
    cost_send[...] = jnp.broadcast_to(0.5 * jnp.sum(part, axis=1, keepdims=True), (1, LANES))

    row_ids = sublane_ids(row_total)
    lane_ids = sublane_ids(2 * LANES)
    once = jnp.minimum(d + 1, 1)

    def looped(body):
        def step(_, carry):
            body()
            return carry

        lax.fori_loop(0, once, step, 0)

    def pack():
        left, right = [], []
        for r in range(obs_rows):
            columns = slice(r * LANES, (r + 1) * LANES)
            values = [halves(coord[c : c + 1, columns]) for c in range(3)]
            values.append(halves(terms[2, r : r + 1, :]))
            tiles = [high for high, _ in values]
            tiles.append(halves(terms[3, r : r + 1, :])[0])
            tiles += [low for _, low in values]
            left.append(spread(one_hot(terms[0, r : r + 1, :], row_ids), tiles))
            right.append(jnp.concatenate(one_hot(terms[1, r : r + 1, :], lane_ids), axis=0))
        packed = dot_nt(jnp.concatenate(left, axis=1), jnp.concatenate(right, axis=1))
        for p in range(dev_count):
            lanes = slice(p // half_dev * LANES, (p // half_dev + 1) * LANES)
            for c in range(CHANNELS):
                start = c * row_total + p % half_dev * per_dest
                rows = packed[start : start + per_dest, lanes]
                if c < 4:
                    start = (c + CHANNELS) * row_total + p % half_dev * per_dest
                    rows = rows + packed[start : start + per_dest, lanes]
                send[p, c * per_dest : (c + 1) * per_dest, :] = rows

    looped(pack)

    def data_copy(p, source):
        return pltpu.make_async_remote_copy(
            src_ref=send.at[p], dst_ref=recv.at[source],
            send_sem=send_sem.at[p], recv_sem=recv_sem.at[source],
            device_id=(g, p), device_id_type=MESH,
        )

    def cost_copy(p, source):
        return pltpu.make_async_remote_copy(
            src_ref=cost_send, dst_ref=cost_recv.at[source],
            send_sem=cost_send_sem.at[p], recv_sem=cost_recv_sem.at[source],
            device_id=(g, p), device_id_type=MESH,
        )

    def group_copy(j):
        return pltpu.make_async_remote_copy(
            src_ref=group_send, dst_ref=group_recv.at[j],
            send_sem=group_send_sem.at[j], recv_sem=group_recv_sem.at[j],
            device_id=wrapped(j, 0), device_id_type=MESH,
        )

    own = d // batch

    def send_to(p):
        when(p > d, lambda: pl.semaphore_wait(up_sem.at[p], 1))
        data_copy(p, d).start()
        cost_copy(p, d).start()

    late = dev_count - batch
    for p in range(late):
        when(p != d, lambda: send_to(p))
    for p in range(late, dev_count):
        when((own >= BATCHES - 2) & (p != d), lambda: send_to(p))
    recv[d] = send[d]

    elem_ids = sublane_ids(ELEM_DEV)
    rows = batch * per_dest

    def prepare(x):
        def channel(c):
            start = c * per_dest
            parts = [recv[x * batch + i, start : start + per_dest, :] for i in range(batch)]
            return jnp.concatenate(parts, axis=0)

        weighted = [first * channel(3) for first in basis_values(channel(0))]
        second = basis_values(channel(1))
        for c, value in enumerate(basis_values(channel(2))):
            third[c * rows : (c + 1) * rows, :] = value
        for i, (a, b) in enumerate(PAIRS):
            outer[i] = weighted[a] * second[b]

    def pair_sums(x, groups):
        left, right = [], []
        for h in range(rows):
            w = third[pl.ds(h, 8, stride=rows), :]
            pieces = []
            for start, stop in groups:
                highs, lows = [], []
                for i in range(start, stop, 2):
                    value = jnp.concatenate([outer[k, h : h + 1, :] * w for k in (i, i + 1)], axis=0)
                    high = value.astype(BF16)
                    highs.append(high)
                    lows.append((value - high.astype(F32)).astype(BF16))
                pieces += highs + lows
            left.append(jnp.concatenate(pieces, axis=0))
            start = 4 * per_dest + h % per_dest
            owner = recv[x * batch + h // per_dest, start : start + 1, :]
            right.append(jnp.concatenate(one_hot(owner, elem_ids), axis=0))
        total = dot_nt(jnp.concatenate(left, axis=1), jnp.concatenate(right, axis=1))
        sums, row = [], 0
        for start, stop in groups:
            count = (stop - start) * 8
            sums.append(total[row : row + count] + total[row + count : row + 2 * count])
            row += 2 * count
        return sums

    faces, inners = (0, len(OUTER_PAIRS)), (len(OUTER_PAIRS), len(PAIRS))

    def arrive(source):
        data_copy(source, source).wait_recv()

    for i in range(batch):
        when(own * batch + i != d, lambda: arrive(own * batch + i))

    def first_sums():
        prepare(own)
        face_rows[...], inner_rows[...] = pair_sums(own, (faces, inners))

    looped(first_sums)

    for p in range(late, dev_count):
        when(own < BATCHES - 2, lambda: send_to(p))

    def from_batch(t):
        x = t - 1 + (t > own).astype(jnp.int32)
        for i in range(batch):
            arrive(x * batch + i)
        prepare(x)
        return x

    def middle(t, carry):
        face, inner = pair_sums(from_batch(t), (faces, inners))
        face_rows[...] += face
        inner_rows[...] += inner
        return carry

    lax.fori_loop(1, BATCHES - 1, middle, 0)
    last = from_batch(BATCHES - 1)

    def place(value, pairs):
        for i, (a, b) in enumerate(pairs):
            start = a * 64 + b * 8
            raw[start : start + 8, :] = value[i * 8 : i * 8 + 8]

    looped(lambda: place(face_rows[...] + pair_sums(last, (faces,))[0], OUTER_PAIRS))

    lane = lax.broadcasted_iota(jnp.int32, (1, LANES), 1)
    lower_half = lane < 64
    node = (lane // 8) % 8
    block = raw[448:512, 128:256]
    a_send[0] = jnp.where(lower_half, pltpu.roll(block[0:32], 64, 1), block[32:64])
    block = raw[0:64, 0:128]
    a_send[1] = jnp.where(lower_half, block[0:32], pltpu.roll(block[32:64], 64, 1))
    for half in range(2):
        columns = slice(half * LANES, (half + 1) * LANES)
        up = pltpu.roll(raw[56:64, columns], 72, 1)
        down = raw[0:8, columns]
        for a in range(1, 8):
            high = raw[a * 64 + 56 : a * 64 + 64, columns]
            low = raw[a * 64 : a * 64 + 8, columns]
            up = jnp.where(node == a, pltpu.roll(high, (a * 8 + 72) % 128, 1), up)
            down = jnp.where(node == a, pltpu.roll(low, a * 8, 1), down)
        b_send[0, half] = up
        b_send[1, half] = down

    steps = (1, -1)

    def face_copy(i):
        if i < 2:
            source, sink, target = a_send.at[i], a_recv.at[i], wrapped(steps[i], 0)
        else:
            source, sink, target = b_send.at[i - 2], b_recv.at[i - 2], wrapped(0, steps[i - 2])
        return pltpu.make_async_remote_copy(
            src_ref=source, dst_ref=sink,
            send_sem=face_send_sem.at[i], recv_sem=face_recv_sem.at[i],
            device_id=target, device_id_type=MESH,
        )

    def edge_copy(i, j):
        return pltpu.make_async_remote_copy(
            src_ref=b_send.at[j, 1 - i], dst_ref=edge_recv.at[j, i],
            send_sem=edge_send_sem.at[j, i], recv_sem=edge_recv_sem.at[j, i],
            device_id=wrapped(steps[i], steps[j]), device_id_type=MESH,
        )

    sends_a, sends_b = (g < grp_count - 1, g > 0), (d < dev_count - 1, d > 0)
    gets_a, gets_b = (g > 0, g < grp_count - 1), (d > 0, d < dev_count - 1)

    def clear(ref, i):
        ref[i] = jnp.zeros_like(ref[i])

    when(higher_others > 0, lambda: pl.semaphore_wait(others_sem, higher_others))
    for j in range(2):
        for i in range(2):
            when(sends_a[i] & sends_b[j], lambda: edge_copy(i, j).start())
    for i in range(2):
        when(sends_a[i], lambda: face_copy(i).start())
        when(sends_b[i], lambda: face_copy(2 + i).start())

    group_cost = cost_send[...]
    for i in range(dev_count):
        when(i != d, lambda: cost_copy(i, i).wait_recv())
        group_cost = group_cost + jnp.where(i == d, 0.0, cost_recv[i])
    group_send[...] = group_cost
    for j in range(1, grp_count):
        group_copy(j).start()

    looped(lambda: place(inner_rows[...] + pair_sums(last, (inners,))[0], INNER_PAIRS))

    for i in range(2):
        when(gets_a[i], lambda: face_copy(i).wait_recv())
        when(jnp.logical_not(gets_a[i]), lambda: clear(a_recv, i))
    low, high = raw[0:64, :], raw[448:512, :]
    from_low, from_high = a_recv[0], a_recv[1]
    from_low = jnp.concatenate([from_low, pltpu.roll(from_low, 64, 1)], axis=0)
    from_high = jnp.concatenate([pltpu.roll(from_high, 64, 1), from_high], axis=0)
    high_rolled = [pltpu.roll(high[:, :128], 64, 1), pltpu.roll(high[:, 128:], 64, 1)]
    low_rolled = [pltpu.roll(low[:, :128], 64, 1), pltpu.roll(low[:, 128:], 64, 1)]
    raw[0:64, 0:128] = low[:, :128] + jnp.where(lower_half, from_low, high_rolled[0])
    raw[0:64, 128:256] = low[:, 128:] + jnp.where(lower_half, high_rolled[0], high_rolled[1])
    raw[448:512, 0:128] = high[:, :128] + jnp.where(lower_half, low_rolled[0], low_rolled[1])
    raw[448:512, 128:256] = high[:, 128:] + jnp.where(lower_half, low_rolled[1], from_high)

    faces = []
    for j in range(2):
        when(gets_b[j], lambda: face_copy(2 + j).wait_recv())
        when(jnp.logical_not(gets_b[j]), lambda: clear(b_recv, j))
        for i in range(2):
            both = gets_a[i] & gets_b[j]
            when(both, lambda: edge_copy(i, j).wait_recv())
            when(jnp.logical_not(both), lambda: clear(edge_recv, (j, i)))
        first, second = b_recv[j, 0], b_recv[j, 1]
        up = [pltpu.roll(x, 8, 1) for x in (edge_recv[j, 0], first, second)]
        down = [pltpu.roll(x, 120, 1) for x in (first, second, edge_recv[j, 1])]
        face = []
        for half, own in enumerate((first, second)):
            from_low = jnp.where(lower_half, up[half], up[half + 1])
            from_high = jnp.where(lower_half, down[half], down[half + 1])
            face.append(
                own + jnp.where(node == 0, from_low, jnp.where(node == 7, from_high, 0.0))
            )
        faces.append(face)
    for half in range(2):
        columns = slice(half * LANES, (half + 1) * LANES)
        for a in range(8):
            low_rows = slice(a * 64, a * 64 + 8)
            high_rows = slice(a * 64 + 56, a * 64 + 64)
            low, high = raw[low_rows, columns], raw[high_rows, columns]
            got_low = pltpu.roll(faces[0][half], (128 - a * 8) % 128, 1)
            got_high = pltpu.roll(faces[1][half], (56 - a * 8) % 128, 1)
            raw[low_rows, columns] = low + jnp.where(node == 0, got_low, pltpu.roll(high, 8, 1))
            raw[high_rows, columns] = high + jnp.where(node == 7, got_high, pltpu.roll(low, 120, 1))

    ez = lax.broadcasted_iota(jnp.int32, (1, 8, LANES), 2) % 8
    c = lax.broadcasted_iota(jnp.int32, (1, 8, LANES), 1)
    takes_low = (c == 0) & (ez > 0)
    takes_high = (c == 7) & (ez < 7)
    for half in range(2):
        for part in range(4):
            rows = slice(part * 128, (part + 1) * 128)
            field = raw[rows, half * LANES : (half + 1) * LANES].reshape(16, 8, LANES)
            below = pltpu.roll(pltpu.roll(field, 1, 2), 1, 1)
            above = pltpu.roll(pltpu.roll(field, 127, 2), 7, 1)
            field = field + jnp.where(takes_low, below, jnp.where(takes_high, above, 0.0))
            out[half * LANES : (half + 1) * LANES, rows] = field.reshape(128, LANES).T

    all_cost = group_send[...]
    for j in range(1, grp_count):
        group_copy(j).wait_recv()
        all_cost = all_cost + group_recv[j]
    cost[...] = all_cost

    for p in range(dev_count):
        when(p != d, lambda: data_copy(p, p).wait_send())
        when(p != d, lambda: cost_copy(p, p).wait_send())
    for j in range(1, grp_count):
        group_copy(j).wait_send()
    for i in range(2):
        when(sends_a[i], lambda: face_copy(i).wait_send())
        when(sends_b[i], lambda: face_copy(2 + i).wait_send())
        for j in range(2):
            when(sends_a[i] & sends_b[j], lambda: edge_copy(i, j).wait_send())


def on_device(obs_coord, obs_resid, obs_weight, obs_dest, obs_send_slot, obs_elem, obs_slot):
    dev_count = lax.axis_size("dev")
    grp_count = lax.axis_size("grp")
    row_count = obs_resid.shape[0]
    obs_rows = row_count // LANES
    capacity = 2 * row_count // dev_count
    per_dest = capacity // LANES
    batch_rows = dev_count // BATCHES * per_dest
    vmem = pl.BlockSpec(memory_space=pltpu.VMEM)
    dma = pltpu.SemaphoreType.DMA
    regular = pltpu.SemaphoreType.REGULAR
    rows = [
        x.reshape(obs_rows, LANES)
        for x in (obs_resid, obs_weight, obs_dest, obs_send_slot, obs_elem)
    ]
    field, cost = pl.pallas_call(
        functools.partial(kernel, dev_count, grp_count, capacity),
        out_shape=(
            pltpu.VMEM((ELEM_DEV, 512), F32),
            pltpu.VMEM((1, LANES), F32),
        ),
        in_specs=[pl.BlockSpec(memory_space=pl.ANY)] * 6,
        out_specs=(vmem, vmem),
        scratch_shapes=[
            pltpu.VMEM((3, row_count), F32),
            pltpu.VMEM((obs_rows, LANES), F32),
            pltpu.VMEM((obs_rows, LANES), F32),
            pltpu.VMEM((obs_rows, LANES), jnp.int32),
            pltpu.VMEM((obs_rows, LANES), jnp.int32),
            pltpu.VMEM((obs_rows, LANES), jnp.int32),
            pltpu.VMEM((4, obs_rows, LANES), F32),
            pltpu.VMEM((dev_count, CHANNELS * per_dest, LANES), F32),
            pltpu.VMEM((dev_count, CHANNELS * per_dest, LANES), F32),
            pltpu.VMEM((1, LANES), F32),
            pltpu.VMEM((dev_count, 1, LANES), F32),
            pltpu.VMEM((1, LANES), F32),
            pltpu.VMEM((grp_count, 1, LANES), F32),
            pltpu.VMEM((64, batch_rows, LANES), F32),
            pltpu.VMEM((8 * batch_rows, LANES), F32),
            pltpu.VMEM((len(OUTER_PAIRS) * 8, ELEM_DEV), F32),
            pltpu.VMEM((len(INNER_PAIRS) * 8, ELEM_DEV), F32),
            pltpu.VMEM((512, ELEM_DEV), F32),
            pltpu.VMEM((2, 32, LANES), F32),
            pltpu.VMEM((2, 32, LANES), F32),
            pltpu.VMEM((2, 2, 8, LANES), F32),
            pltpu.VMEM((2, 2, 8, LANES), F32),
            pltpu.VMEM((2, 2, 8, LANES), F32),
            dma((dev_count,)),
            dma((dev_count,)),
            dma((dev_count,)),
            dma((dev_count,)),
            dma((grp_count,)),
            dma((grp_count,)),
            dma((4,)),
            dma((4,)),
            dma((2, 2)),
            dma((2, 2)),
            dma((6,)),
            regular((dev_count,)),
            regular,
        ],
        compiler_params=pltpu.CompilerParams(collective_id=0, has_side_effects=True),
    )(obs_coord, *rows)
    return field.reshape(EX, EY, EZ, 512), cost[0, 0]


def solution(mesh):
    placed = (
        P(None, ("grp", "dev")),
        P(("grp", "dev")),
        P(("grp", "dev")),
        P(("grp", "dev")),
        P(("grp", "dev")),
        P(("grp", "dev")),
        P(("grp", "dev")),
    )
    return jax.shard_map(
        on_device,
        mesh=mesh,
        in_specs=placed,
        out_specs=(P("grp", "dev", None, None), P()),
        check_vma=False,
    )
```

```python
import functools
import math

import jax
import jax.numpy as jnp
from jax import lax
from jax.experimental import pallas as pl
from jax.experimental.pallas import tpu as pltpu
from jax.sharding import PartitionSpec as P

EX = 4
EY = 8
EZ = 8
ELEM_DEV = 256
LANES = 128
CHANNELS = 5
BATCHES = 4
MESH = pl.DeviceIdType.MESH
F32 = jnp.float32
BF16 = jnp.bfloat16
F8 = jnp.float8_e4m3fn

ANCHORS = [-math.cos(math.pi * k / 7) for k in range(8)]
OUTER_PAIRS = [(a, b) for a in (0, 7) for b in range(8)]
OUTER_PAIRS += [(a, b) for a in range(1, 7) for b in (0, 7)]
INNER_PAIRS = [(a, b) for a in range(1, 7) for b in range(1, 7)]
PAIRS = OUTER_PAIRS + INNER_PAIRS
COEFS = [
    1.0 / math.prod(ANCHORS[a] - ANCHORS[m] for m in range(8) if m != a) for a in range(8)
]


def basis_values(t):
    factors = [t - p for p in ANCHORS]
    prefix = [None] * 8
    suffix = [None] * 8
    for k in range(1, 8):
        prefix[k] = factors[k - 1] if k == 1 else prefix[k - 1] * factors[k - 1]
    for k in range(6, -1, -1):
        suffix[k] = factors[k + 1] if k == 6 else suffix[k + 1] * factors[k + 1]
    basis = []
    for a in range(8):
        if a == 0:
            product = suffix[0]
        elif a == 7:
            product = prefix[7]
        else:
            product = prefix[a] * suffix[a]
        basis.append(product * COEFS[a])
    return basis


def dot_nt(left, right):
    return lax.dot_general(left, right, (((1,), (1,)), ((), ())), preferred_element_type=F32)


def halves(row):
    value = jnp.broadcast_to(row, (16, LANES))
    first = value.astype(BF16)
    return first, (value - first.astype(F32)).astype(BF16)


def one_hot(row, ids):
    tile = jnp.broadcast_to(row, (ids[0].shape[0], LANES)).astype(BF16)
    return [jnp.where(part == tile, jnp.ones((), BF16), jnp.zeros((), BF16)) for part in ids]


def spread(hot, tiles):
    return jnp.concatenate([part * tile for tile in tiles for part in hot], axis=0)


def sublane_ids(count, step=16):
    ids = lax.broadcasted_iota(jnp.int32, (step, LANES), 0)
    return [(ids + step * i).astype(F32).astype(BF16) for i in range(count // step)]


def kernel(
    dev_count, grp_count, capacity,
    coord_in, resid_in, weight_in, dest_in, slot_in, elem_in,
    out, cost,
    coord, resid, weight, dest, slot, elem, terms, send, recv,
    group_send, group_recv,
    outer, third, face_rows, inner_rows, raw, a_send, a_recv, b_send, b_recv, edge_recv,
    send_sem, recv_sem, group_send_sem, group_recv_sem,
    face_send_sem, face_recv_sem, edge_send_sem, edge_recv_sem, load_sem,
    up_sem, others_sem,
):
    g = lax.axis_index("grp")
    d = lax.axis_index("dev")
    obs_rows = resid.shape[0]
    per_dest = capacity // LANES
    half_dev = dev_count // 2
    quarter_dev = half_dev // 2
    row_total = quarter_dev * per_dest
    batch = dev_count // BATCHES

    def when(condition, action):
        @pl.when(condition)
        def _():
            action()

    def wrapped(step_g, step_d):
        return (
            lax.rem(g + step_g + grp_count, grp_count),
            lax.rem(d + step_d + dev_count, dev_count),
        )

    loads = [
        pltpu.make_async_copy(source, sink, load_sem.at[i])
        for i, (source, sink) in enumerate(
            zip(
                (dest_in, slot_in, resid_in, weight_in, coord_in, elem_in),
                (dest, slot, resid, weight, coord, elem),
            )
        )
    ]
    for load in loads:
        load.start()

    barrier = pltpu.get_barrier_semaphore()
    others = [wrapped(j, 0) for j in range(1, grp_count)]
    others += [wrapped(i, j) for i in (-1, 1) for j in (-1, 1)]

    def signal(semaphore, partner):
        pl.semaphore_signal(semaphore, inc=1, device_id=partner, device_id_type=MESH)

    def is_lower(partner):
        return (partner[1] < d) | ((partner[1] == d) & (partner[0] < g))

    for p in range(dev_count):
        when(p > d, lambda: signal(barrier, (g, p)))
    lower_count = d
    higher_others = len(others)
    for partner in others:
        lower = is_lower(partner)
        when(jnp.logical_not(lower), lambda: signal(barrier, partner))
        lower_count = lower_count + lower.astype(jnp.int32)
        higher_others = higher_others - lower.astype(jnp.int32)
    for load in loads:
        load.wait()

    residual = resid[...]
    forcing = weight[...] * residual
    where = dest[...]
    which = slot[...]
    row = where % quarter_dev * per_dest + which // LANES
    for half in range(2):
        terms[half] = jnp.where(where // half_dev == half, row, -1).astype(F32)
    terms[2] = (where // quarter_dev % 2 * LANES + which % LANES).astype(F32)
    terms[3] = forcing
    terms[4] = elem[...].astype(F32)
    part = jnp.sum(forcing * residual, axis=0, keepdims=True)
    part = jnp.broadcast_to(0.5 * jnp.sum(part, axis=1, keepdims=True), (1, LANES))
    cost_row = slice(CHANNELS * per_dest, CHANNELS * per_dest + 1)
    for p in range(dev_count):
        send[p, cost_row, :] = part

    row_ids = sublane_ids(row_total)
    lane_ids = sublane_ids(2 * LANES, 32)
    once = jnp.minimum(d + 1, 1)

    def looped(body):
        def step(_, carry):
            body()
            return carry

        lax.fori_loop(0, once, step, 0)

    def pack(half):
        left, right = [], []
        for r in range(obs_rows):
            columns = slice(r * LANES, (r + 1) * LANES)
            values = [halves(coord[c : c + 1, columns]) for c in range(3)]
            values.append(halves(terms[3, r : r + 1, :]))
            tiles = [high for high, _ in values]
            tiles.append(halves(terms[4, r : r + 1, :])[0])
            tiles += [low for _, low in values]
            left.append(spread(one_hot(terms[half, r : r + 1, :], row_ids), tiles))
            hot = one_hot(terms[2, r : r + 1, :], lane_ids)
            right.append(jnp.concatenate([part.astype(F8) for part in hot], axis=0))
        packed = dot_nt(jnp.concatenate(left, axis=1), jnp.concatenate(right, axis=1))
        for q in range(half_dev):
            lanes = slice(q // quarter_dev * LANES, (q // quarter_dev + 1) * LANES)
            for c in range(CHANNELS):
                start = c * row_total + q % quarter_dev * per_dest
                rows = packed[start : start + per_dest, lanes]
                if c < 4:
                    start = (c + CHANNELS) * row_total + q % quarter_dev * per_dest
                    rows = rows + packed[start : start + per_dest, lanes]
                send[half * half_dev + q, c * per_dest : (c + 1) * per_dest, :] = rows

    def data_copy(p, source):
        return pltpu.make_async_remote_copy(
            src_ref=send.at[p], dst_ref=recv.at[source],
            send_sem=send_sem.at[p], recv_sem=recv_sem.at[source],
            device_id=(g, p), device_id_type=MESH,
        )

    def group_copy(j):
        return pltpu.make_async_remote_copy(
            src_ref=group_send, dst_ref=group_recv.at[j],
            send_sem=group_send_sem.at[j], recv_sem=group_recv_sem.at[j],
            device_id=wrapped(j, 0), device_id_type=MESH,
        )

    own = d // batch

    def send_to(p):
        when(p > d, lambda: pl.semaphore_wait(up_sem.at[p], 1))
        data_copy(p, d).start()

    looped(lambda: pack(0))
    when(lower_count > 0, lambda: pl.semaphore_wait(barrier, lower_count))
    for p in range(dev_count):
        when(p < d, lambda: signal(up_sem.at[d], (g, p)))
    for partner in others:
        when(is_lower(partner), lambda: signal(others_sem, partner))

    for p in range(half_dev):
        when(p < d, lambda: send_to(p))
    looped(lambda: pack(1))
    for p in range(half_dev, dev_count):
        when(p < d, lambda: send_to(p))
    for i in range(batch):
        when(own * batch + i > d, lambda: send_to(own * batch + i))
    recv[d] = send[d]

    elem_ids = sublane_ids(ELEM_DEV)
    rows = batch * per_dest

    def prepare(x):
        def channel(c):
            start = c * per_dest
            parts = [recv[x * batch + i, start : start + per_dest, :] for i in range(batch)]
            return jnp.concatenate(parts, axis=0)

        weighted = [first * channel(3) for first in basis_values(channel(0))]
        second = basis_values(channel(1))
        for c, value in enumerate(basis_values(channel(2))):
            third[c * rows : (c + 1) * rows, :] = value
        for i, (a, b) in enumerate(PAIRS):
            outer[i] = weighted[a] * second[b]

    def pair_sums(x, groups):
        left, right = [], []
        for h in range(rows):
            w = third[pl.ds(h, 8, stride=rows), :]
            pieces = []
            for start, stop in groups:
                highs, lows = [], []
                for i in range(start, stop, 2):
                    value = jnp.concatenate([outer[k, h : h + 1, :] * w for k in (i, i + 1)], axis=0)
                    high = value.astype(BF16)
                    highs.append(high)
                    lows.append((value - high.astype(F32)).astype(BF16))
                pieces += highs + lows
            left.append(jnp.concatenate(pieces, axis=0))
            start = 4 * per_dest + h % per_dest
            owner = recv[x * batch + h // per_dest, start : start + 1, :]
            right.append(jnp.concatenate(one_hot(owner, elem_ids), axis=0))
        total = dot_nt(jnp.concatenate(left, axis=1), jnp.concatenate(right, axis=1))
        sums, row = [], 0
        for start, stop in groups:
            count = (stop - start) * 8
            sums.append(total[row : row + count] + total[row + count : row + 2 * count])
            row += 2 * count
        return sums

    faces, inners = (0, len(OUTER_PAIRS)), (len(OUTER_PAIRS), len(PAIRS))

    def arrive(source):
        data_copy(source, source).wait_recv()

    for i in range(batch):
        when(own * batch + i != d, lambda: arrive(own * batch + i))

    def first_sums():
        prepare(own)
        face_rows[...], inner_rows[...] = pair_sums(own, (faces, inners))

    looped(first_sums)

    def send_up(x):
        for i in range(batch):
            when(x < BATCHES, lambda: send_to(x * batch + i))

    send_up(own + 1)
    send_up(own + 2)

    def from_batch(t):
        early = own < BATCHES // 2
        turn = jnp.where(early, own, BATCHES - 1 - own)
        x = t - 1 + (t > turn).astype(jnp.int32)
        x = jnp.where(early, x, BATCHES - 1 - x)
        for i in range(batch):
            arrive(x * batch + i)
        prepare(x)
        return x

    def middle(t, carry):
        for j in range(3, BATCHES):
            when(t == j - 1, lambda: send_up(own + j))
        face, inner = pair_sums(from_batch(t), (faces, inners))
        face_rows[...] += face
        inner_rows[...] += inner
        return carry

    lax.fori_loop(1, BATCHES - 1, middle, 0)
    last = from_batch(BATCHES - 1)
    when(higher_others > 0, lambda: pl.semaphore_wait(others_sem, higher_others))
    group_cost = recv[0, cost_row, :]
    for i in range(1, dev_count):
        group_cost = group_cost + recv[i, cost_row, :]
    group_send[...] = group_cost
    for j in range(1, grp_count):
        group_copy(j).start()

    def place(value, pairs):
        for i, (a, b) in enumerate(pairs):
            start = a * 64 + b * 8
            for half in range(2):
                lanes = slice(half * LANES, (half + 1) * LANES)
                raw[half, start : start + 8, :] = value[i * 8 : i * 8 + 8, lanes]

    looped(lambda: place(face_rows[...] + pair_sums(last, (faces,))[0], OUTER_PAIRS))

    lane = lax.broadcasted_iota(jnp.int32, (1, LANES), 1)
    lower_half = lane < 64
    node = (lane // 8) % 8
    block = raw[1, 448:512, :]
    a_send[0] = jnp.where(lower_half, pltpu.roll(block[0:32], 64, 1), block[32:64])
    block = raw[0, 0:64, :]
    a_send[1] = jnp.where(lower_half, block[0:32], pltpu.roll(block[32:64], 64, 1))
    for half in range(2):
        up = pltpu.roll(raw[half, 56:64, :], 72, 1)
        down = raw[half, 0:8, :]
        for a in range(1, 8):
            high = raw[half, a * 64 + 56 : a * 64 + 64, :]
            low = raw[half, a * 64 : a * 64 + 8, :]
            up = jnp.where(node == a, pltpu.roll(high, (a * 8 + 72) % 128, 1), up)
            down = jnp.where(node == a, pltpu.roll(low, a * 8, 1), down)
        b_send[0, half] = up
        b_send[1, half] = down

    steps = (1, -1)

    def face_copy(i):
        if i < 2:
            source, sink, target = a_send.at[i], a_recv.at[i], wrapped(steps[i], 0)
        else:
            source, sink, target = b_send.at[i - 2], b_recv.at[i - 2], wrapped(0, steps[i - 2])
        return pltpu.make_async_remote_copy(
            src_ref=source, dst_ref=sink,
            send_sem=face_send_sem.at[i], recv_sem=face_recv_sem.at[i],
            device_id=target, device_id_type=MESH,
        )

    def edge_copy(i, j):
        return pltpu.make_async_remote_copy(
            src_ref=b_send.at[j, 1 - i], dst_ref=edge_recv.at[j, i],
            send_sem=edge_send_sem.at[j, i], recv_sem=edge_recv_sem.at[j, i],
            device_id=wrapped(steps[i], steps[j]), device_id_type=MESH,
        )

    sends_a, sends_b = (g < grp_count - 1, g > 0), (d < dev_count - 1, d > 0)
    gets_a, gets_b = (g > 0, g < grp_count - 1), (d > 0, d < dev_count - 1)

    def clear(ref, i):
        ref[i] = jnp.zeros_like(ref[i])

    for j in range(2):
        for i in range(2):
            when(sends_a[i] & sends_b[j], lambda: edge_copy(i, j).start())
    for i in range(2):
        when(sends_a[i], lambda: face_copy(i).start())
        when(sends_b[i], lambda: face_copy(2 + i).start())

    looped(lambda: place(inner_rows[...] + pair_sums(last, (inners,))[0], INNER_PAIRS))

    low_rows, high_rows = slice(0, 64), slice(448, 512)
    low = [raw[half, low_rows, :] for half in range(2)]
    high = [raw[half, high_rows, :] for half in range(2)]
    low_rolled = [pltpu.roll(x, 64, 1) for x in low]
    high_rolled = [pltpu.roll(x, 64, 1) for x in high]
    raw[0, low_rows, :] = low[0] + jnp.where(lower_half, 0.0, high_rolled[0])
    raw[1, low_rows, :] = low[1] + jnp.where(lower_half, high_rolled[0], high_rolled[1])
    raw[0, high_rows, :] = high[0] + jnp.where(lower_half, low_rolled[0], low_rolled[1])
    raw[1, high_rows, :] = high[1] + jnp.where(lower_half, low_rolled[1], 0.0)

    def from_below(high):
        return jnp.where(node == 0, 0.0, pltpu.roll(high, 8, 1))

    def from_above(low):
        return jnp.where(node == 7, 0.0, pltpu.roll(low, 120, 1))

    for half in range(2):
        for a in range(8):
            low_rows, high_rows = slice(a * 64, a * 64 + 8), slice(a * 64 + 56, a * 64 + 64)
            low, high = raw[half, low_rows, :], raw[half, high_rows, :]
            raw[half, low_rows, :] = low + from_below(high)
            raw[half, high_rows, :] = high + from_above(low)

    for i in range(2):
        when(gets_a[i], lambda: face_copy(i).wait_recv())
        when(jnp.logical_not(gets_a[i]), lambda: clear(a_recv, i))
    for i in range(2):
        got = a_recv[i]
        parts = [got, pltpu.roll(got, 64, 1)]
        if i == 0:
            got = jnp.where(lower_half, jnp.concatenate(parts, axis=0), 0.0)
        else:
            got = jnp.where(lower_half, 0.0, jnp.concatenate(parts[::-1], axis=0))
        start = i * 448
        raw[i, start : start + 8, :] += got[0:8] + from_below(got[56:64])
        raw[i, start + 8 : start + 56, :] += got[8:56]
        raw[i, start + 56 : start + 64, :] += got[56:64] + from_above(got[0:8])

    faces = []
    for j in range(2):
        when(gets_b[j], lambda: face_copy(2 + j).wait_recv())
        when(jnp.logical_not(gets_b[j]), lambda: clear(b_recv, j))
        for i in range(2):
            both = gets_a[i] & gets_b[j]
            when(both, lambda: edge_copy(i, j).wait_recv())
            when(jnp.logical_not(both), lambda: clear(edge_recv, (j, i)))
        first, second = b_recv[j, 0], b_recv[j, 1]
        up = [pltpu.roll(x, 8, 1) for x in (edge_recv[j, 0], first, second)]
        down = [pltpu.roll(x, 120, 1) for x in (first, second, edge_recv[j, 1])]
        face = []
        for half, own in enumerate((first, second)):
            from_low = jnp.where(lower_half, up[half], up[half + 1])
            from_high = jnp.where(lower_half, down[half], down[half + 1])
            face.append(
                own + jnp.where(node == 0, from_low, jnp.where(node == 7, from_high, 0.0))
            )
        faces.append(face)
    for half in range(2):
        for a in range(8):
            low_rows, high_rows = slice(a * 64, a * 64 + 8), slice(a * 64 + 56, a * 64 + 64)
            got_low = pltpu.roll(faces[0][half], (128 - a * 8) % 128, 1)
            got_high = pltpu.roll(faces[1][half], (56 - a * 8) % 128, 1)
            raw[half, low_rows, :] += jnp.where(node == 0, got_low, 0.0)
            raw[half, high_rows, :] += jnp.where(node == 7, got_high, 0.0)

    ez = lane % 8
    for half in range(2):
        for a in range(8):
            low_rows = pl.ds(a * 64, 8, stride=8)
            high_rows = pl.ds(a * 64 + 7, 8, stride=8)
            low, high = raw[half, low_rows, :], raw[half, high_rows, :]
            raw[half, low_rows, :] = low + jnp.where(ez > 0, pltpu.roll(high, 1, 1), 0.0)
            raw[half, high_rows, :] = high + jnp.where(ez < 7, pltpu.roll(low, 127, 1), 0.0)
        for part in range(4):
            rows = slice(part * 128, (part + 1) * 128)
            out[half * LANES : (half + 1) * LANES, rows] = raw[half, rows, :].T

    all_cost = group_send[...]
    for j in range(1, grp_count):
        group_copy(j).wait_recv()
        all_cost = all_cost + group_recv[j]
    cost[...] = all_cost

    for p in range(dev_count):
        when(p != d, lambda: data_copy(p, p).wait_send())
    for j in range(1, grp_count):
        group_copy(j).wait_send()
    for i in range(2):
        when(sends_a[i], lambda: face_copy(i).wait_send())
        when(sends_b[i], lambda: face_copy(2 + i).wait_send())
        for j in range(2):
            when(sends_a[i] & sends_b[j], lambda: edge_copy(i, j).wait_send())


def on_device(obs_coord, obs_resid, obs_weight, obs_dest, obs_send_slot, obs_elem, obs_slot):
    dev_count = lax.axis_size("dev")
    grp_count = lax.axis_size("grp")
    row_count = obs_resid.shape[0]
    obs_rows = row_count // LANES
    capacity = 2 * row_count // dev_count
    per_dest = capacity // LANES
    batch_rows = dev_count // BATCHES * per_dest
    vmem = pl.BlockSpec(memory_space=pltpu.VMEM)
    dma = pltpu.SemaphoreType.DMA
    regular = pltpu.SemaphoreType.REGULAR
    rows = [
        x.reshape(obs_rows, LANES)
        for x in (obs_resid, obs_weight, obs_dest, obs_send_slot, obs_elem)
    ]
    field, cost = pl.pallas_call(
        functools.partial(kernel, dev_count, grp_count, capacity),
        out_shape=(
            pltpu.VMEM((ELEM_DEV, 512), F32),
            pltpu.VMEM((1, LANES), F32),
        ),
        in_specs=[pl.BlockSpec(memory_space=pl.ANY)] * 6,
        out_specs=(vmem, vmem),
        scratch_shapes=[
            pltpu.VMEM((3, row_count), F32),
            pltpu.VMEM((obs_rows, LANES), F32),
            pltpu.VMEM((obs_rows, LANES), F32),
            pltpu.VMEM((obs_rows, LANES), jnp.int32),
            pltpu.VMEM((obs_rows, LANES), jnp.int32),
            pltpu.VMEM((obs_rows, LANES), jnp.int32),
            pltpu.VMEM((5, obs_rows, LANES), F32),
            pltpu.VMEM((dev_count, CHANNELS * per_dest + 1, LANES), F32),
            pltpu.VMEM((dev_count, CHANNELS * per_dest + 1, LANES), F32),
            pltpu.VMEM((1, LANES), F32),
            pltpu.VMEM((grp_count, 1, LANES), F32),
            pltpu.VMEM((64, batch_rows, LANES), F32),
            pltpu.VMEM((8 * batch_rows, LANES), F32),
            pltpu.VMEM((len(OUTER_PAIRS) * 8, ELEM_DEV), F32),
            pltpu.VMEM((len(INNER_PAIRS) * 8, ELEM_DEV), F32),
            pltpu.VMEM((2, 512, LANES), F32),
            pltpu.VMEM((2, 32, LANES), F32),
            pltpu.VMEM((2, 32, LANES), F32),
            pltpu.VMEM((2, 2, 8, LANES), F32),
            pltpu.VMEM((2, 2, 8, LANES), F32),
            pltpu.VMEM((2, 2, 8, LANES), F32),
            dma((dev_count,)),
            dma((dev_count,)),
            dma((grp_count,)),
            dma((grp_count,)),
            dma((4,)),
            dma((4,)),
            dma((2, 2)),
            dma((2, 2)),
            dma((6,)),
            regular((dev_count,)),
            regular,
        ],
        compiler_params=pltpu.CompilerParams(collective_id=0, has_side_effects=True),
    )(obs_coord, *rows)
    return field.reshape(EX, EY, EZ, 512), cost[0, 0]


def solution(mesh):
    placed = (
        P(None, ("grp", "dev")),
        P(("grp", "dev")),
        P(("grp", "dev")),
        P(("grp", "dev")),
        P(("grp", "dev")),
        P(("grp", "dev")),
        P(("grp", "dev")),
    )
    return jax.shard_map(
        on_device,
        mesh=mesh,
        in_specs=placed,
        out_specs=(P("grp", "dev", None, None), P()),
        check_vma=False,
    )
```

```python
import functools
import math

import jax
import jax.numpy as jnp
from jax import lax
from jax.experimental import pallas as pl
from jax.experimental.pallas import tpu as pltpu
from jax.sharding import PartitionSpec as P

EX = 4
EY = 8
EZ = 8
ELEM_DEV = 256
LANES = 128
CHANNELS = 5
BATCHES = 4
MESH = pl.DeviceIdType.MESH
F32 = jnp.float32
BF16 = jnp.bfloat16
F8 = jnp.float8_e4m3fn

ANCHORS = [-math.cos(math.pi * k / 7) for k in range(8)]
OUTER_PAIRS = [(a, b) for a in (0, 7) for b in range(8)]
OUTER_PAIRS += [(a, b) for a in range(1, 7) for b in (0, 7)]
INNER_PAIRS = [(a, b) for a in range(1, 7) for b in range(1, 7)]
PAIRS = OUTER_PAIRS + INNER_PAIRS
COEFS = [
    1.0 / math.prod(ANCHORS[a] - ANCHORS[m] for m in range(8) if m != a) for a in range(8)
]


def basis_values(t):
    factors = [t - p for p in ANCHORS]
    prefix = [None] * 8
    suffix = [None] * 8
    for k in range(1, 8):
        prefix[k] = factors[k - 1] if k == 1 else prefix[k - 1] * factors[k - 1]
    for k in range(6, -1, -1):
        suffix[k] = factors[k + 1] if k == 6 else suffix[k + 1] * factors[k + 1]
    basis = []
    for a in range(8):
        if a == 0:
            product = suffix[0]
        elif a == 7:
            product = prefix[7]
        else:
            product = prefix[a] * suffix[a]
        basis.append(product * COEFS[a])
    return basis


def dot_nt(left, right):
    return lax.dot_general(left, right, (((1,), (1,)), ((), ())), preferred_element_type=F32)


def halves(row):
    value = jnp.broadcast_to(row, (16, LANES))
    first = value.astype(BF16)
    return first, (value - first.astype(F32)).astype(BF16)


def one_hot(row, ids):
    tile = jnp.broadcast_to(row, (ids[0].shape[0], LANES)).astype(BF16)
    return [jnp.where(part == tile, jnp.ones((), BF16), jnp.zeros((), BF16)) for part in ids]


def spread(hot, tiles):
    return jnp.concatenate([part * tile for tile in tiles for part in hot], axis=0)


def sublane_ids(count, step=16):
    ids = lax.broadcasted_iota(jnp.int32, (step, LANES), 0)
    return [(ids + step * i).astype(F32).astype(BF16) for i in range(count // step)]


def kernel(
    dev_count, grp_count, capacity,
    coord_in, resid_in, weight_in, dest_in, slot_in, elem_in,
    out, cost,
    coord, resid, weight, dest, slot, elem, terms, send, recv,
    group_send, group_recv,
    outer, third, face_rows, inner_rows, raw, a_send, a_recv, b_send, b_recv, edge_recv,
    send_sem, recv_sem, group_send_sem, group_recv_sem,
    face_send_sem, face_recv_sem, edge_send_sem, edge_recv_sem, load_sem,
    up_sem, head_sem, ready_sem,
):
    g = lax.axis_index("grp")
    d = lax.axis_index("dev")
    obs_rows = resid.shape[0]
    per_dest = capacity // LANES
    half_dev = dev_count // 2
    quarter_dev = half_dev // 2
    row_total = quarter_dev * per_dest
    batch = dev_count // BATCHES

    def when(condition, action):
        @pl.when(condition)
        def _():
            action()

    def wrapped(step_g, step_d):
        return (
            lax.rem(g + step_g + grp_count, grp_count),
            lax.rem(d + step_d + dev_count, dev_count),
        )

    loads = [
        pltpu.make_async_copy(source, sink, load_sem.at[i])
        for i, (source, sink) in enumerate(
            zip(
                (dest_in, slot_in, resid_in, weight_in, coord_in, elem_in),
                (dest, slot, resid, weight, coord, elem),
            )
        )
    ]
    for load in loads:
        load.start()

    barrier = pltpu.get_barrier_semaphore()
    def signal(semaphore, partner):
        pl.semaphore_signal(semaphore, inc=1, device_id=partner, device_id_type=MESH)

    heads = [wrapped(j, 0) for j in range(1, grp_count)]
    for p in range(dev_count):
        when(p > d, lambda: signal(barrier, (g, p)))
    for head in heads:
        when(d == 0, lambda: signal(barrier, head))
    pl.semaphore_wait(barrier, jnp.where(d == 0, len(heads), d))
    for p in range(dev_count):
        when(p < d, lambda: signal(up_sem.at[d], (g, p)))

    for load in loads:
        load.wait()

    residual = resid[...]
    forcing = weight[...] * residual
    where = dest[...]
    which = slot[...]
    row = where % quarter_dev * per_dest + which // LANES
    for half in range(2):
        terms[half] = jnp.where(where // half_dev == half, row, -1).astype(F32)
    terms[2] = (where // quarter_dev % 2 * LANES + which % LANES).astype(F32)
    terms[3] = forcing
    terms[4] = elem[...].astype(F32)
    part = jnp.sum(forcing * residual, axis=0, keepdims=True)
    part = jnp.broadcast_to(0.5 * jnp.sum(part, axis=1, keepdims=True), (1, LANES))
    cost_row = slice(CHANNELS * per_dest, CHANNELS * per_dest + 1)
    for p in range(dev_count):
        send[p, cost_row, :] = part

    row_ids = sublane_ids(row_total)
    lane_ids = sublane_ids(2 * LANES, 32)
    once = jnp.minimum(d + 1, 1)

    def looped(body):
        def step(_, carry):
            body()
            return carry

        lax.fori_loop(0, once, step, 0)

    def pack(half):
        left, right = [], []
        for r in range(obs_rows):
            columns = slice(r * LANES, (r + 1) * LANES)
            values = [halves(coord[c : c + 1, columns]) for c in range(3)]
            values.append(halves(terms[3, r : r + 1, :]))
            tiles = [high for high, _ in values]
            tiles.append(halves(terms[4, r : r + 1, :])[0])
            tiles += [low for _, low in values]
            left.append(spread(one_hot(terms[half, r : r + 1, :], row_ids), tiles))
            hot = one_hot(terms[2, r : r + 1, :], lane_ids)
            right.append(jnp.concatenate([part.astype(F8) for part in hot], axis=0))
        packed = dot_nt(jnp.concatenate(left, axis=1), jnp.concatenate(right, axis=1))
        for q in range(half_dev):
            lanes = slice(q // quarter_dev * LANES, (q // quarter_dev + 1) * LANES)
            for c in range(CHANNELS):
                start = c * row_total + q % quarter_dev * per_dest
                rows = packed[start : start + per_dest, lanes]
                if c < 4:
                    start = (c + CHANNELS) * row_total + q % quarter_dev * per_dest
                    rows = rows + packed[start : start + per_dest, lanes]
                send[half * half_dev + q, c * per_dest : (c + 1) * per_dest, :] = rows

    def data_copy(p, source):
        return pltpu.make_async_remote_copy(
            src_ref=send.at[p], dst_ref=recv.at[source],
            send_sem=send_sem.at[p], recv_sem=recv_sem.at[source],
            device_id=(g, p), device_id_type=MESH,
        )

    def group_copy(j):
        return pltpu.make_async_remote_copy(
            src_ref=group_send, dst_ref=group_recv.at[j],
            send_sem=group_send_sem.at[j], recv_sem=group_recv_sem.at[j],
            device_id=wrapped(j, 0), device_id_type=MESH,
        )

    own = d // batch

    def send_to(p):
        when(p > d, lambda: pl.semaphore_wait(up_sem.at[p], 1))
        data_copy(p, d).start()

    looped(lambda: pack(0))
    for p in range(half_dev):
        when(p < d, lambda: send_to(p))
    looped(lambda: pack(1))
    for p in range(half_dev, dev_count):
        when(p < d, lambda: send_to(p))
    for i in range(batch):
        when(own * batch + i > d, lambda: send_to(own * batch + i))

    def send_up(x):
        for i in range(batch):
            when(x < BATCHES, lambda: send_to(x * batch + i))

    send_up(own + 1)
    recv[d] = send[d]

    elem_ids = sublane_ids(ELEM_DEV)
    rows = batch * per_dest

    def prepare(x, t):
        def channel(c):
            start = c * per_dest
            parts = [recv[x * batch + i, start : start + per_dest, :] for i in range(batch)]
            return jnp.concatenate(parts, axis=0)

        weighted = [first * channel(3) for first in basis_values(channel(0))]
        second = basis_values(channel(1))
        for c, value in enumerate(basis_values(channel(2))):
            third[t, c * rows : (c + 1) * rows, :] = value
        for i, (a, b) in enumerate(PAIRS):
            outer[t, i] = weighted[a] * second[b]

    def pair_sums(x, t, groups):
        left, right = [], []
        for h in range(rows):
            w = third[t, pl.ds(h, 8, stride=rows), :]
            pieces = []
            for start, stop in groups:
                highs, lows = [], []
                for i in range(start, stop, 2):
                    value = jnp.concatenate([outer[t, k, h : h + 1, :] * w for k in (i, i + 1)], axis=0)
                    high = value.astype(BF16)
                    highs.append(high)
                    lows.append((value - high.astype(F32)).astype(BF16))
                pieces += highs + lows
            left.append(jnp.concatenate(pieces, axis=0))
            start = 4 * per_dest + h % per_dest
            owner = recv[x * batch + h // per_dest, start : start + 1, :]
            right.append(jnp.concatenate(one_hot(owner, elem_ids), axis=0))
        total = dot_nt(jnp.concatenate(left, axis=1), jnp.concatenate(right, axis=1))
        sums, row = [], 0
        for start, stop in groups:
            count = (stop - start) * 8
            sums.append(total[row : row + count] + total[row + count : row + 2 * count])
            row += 2 * count
        return sums

    faces, inners = (0, len(OUTER_PAIRS)), (len(OUTER_PAIRS), len(PAIRS))

    def arrive(source):
        data_copy(source, source).wait_recv()

    for i in range(batch):
        when(own * batch + i != d, lambda: arrive(own * batch + i))

    def first_sums():
        prepare(own, 0)
        face_rows[...], inner_rows[...] = pair_sums(own, 0, (faces, inners))

    looped(first_sums)

    for j in range(2, BATCHES):
        send_up(own + j)
    for head in heads:
        when(d == 0, lambda: signal(head_sem, head))

    def batch_of(t):
        early = own < BATCHES // 2
        turn = jnp.where(early, own, BATCHES - 1 - own)
        x = t - 1 + (t > turn).astype(jnp.int32)
        return jnp.where(early, x, BATCHES - 1 - x)

    def from_batch(t):
        x = batch_of(t)
        for i in range(batch):
            arrive(x * batch + i)
        prepare(x, t)
        return x

    def all_rows(t, carry):
        face, inner = pair_sums(from_batch(t), t, (faces, inners))
        face_rows[...] += face
        inner_rows[...] += inner
        return carry

    def only_faces(t, carry):
        face_rows[...] += pair_sums(from_batch(t), t, (faces,))[0]
        return carry

    def only_inner(t, carry):
        inner_rows[...] += pair_sums(batch_of(t), t, (inners,))[0]
        return carry

    split = jnp.where(own == 0, BATCHES - 2, 1)
    lax.fori_loop(1, split, all_rows, 0)

    @pl.when(d == 0)
    def _():
        pl.semaphore_wait(head_sem, len(heads))
        for p in range(1, dev_count):
            signal(ready_sem, (g, p))

    lax.fori_loop(split, BATCHES - 1, only_faces, 0)
    last = from_batch(BATCHES - 1)
    group_cost = recv[0, cost_row, :]
    for i in range(1, dev_count):
        group_cost = group_cost + recv[i, cost_row, :]
    group_send[...] = group_cost

    def place(value, pairs):
        for i, (a, b) in enumerate(pairs):
            start = a * 64 + b * 8
            for half in range(2):
                lanes = slice(half * LANES, (half + 1) * LANES)
                raw[half, start : start + 8, :] = value[i * 8 : i * 8 + 8, lanes]

    def last_faces():
        place(face_rows[...] + pair_sums(last, BATCHES - 1, (faces,))[0], OUTER_PAIRS)

    looped(last_faces)

    lane = lax.broadcasted_iota(jnp.int32, (1, LANES), 1)
    lower_half = lane < 64
    node = (lane // 8) % 8
    block = raw[1, 448:512, :]
    a_send[0] = jnp.where(lower_half, pltpu.roll(block[0:32], 64, 1), block[32:64])
    block = raw[0, 0:64, :]
    a_send[1] = jnp.where(lower_half, block[0:32], pltpu.roll(block[32:64], 64, 1))
    for half in range(2):
        up = pltpu.roll(raw[half, 56:64, :], 72, 1)
        down = raw[half, 0:8, :]
        for a in range(1, 8):
            high = raw[half, a * 64 + 56 : a * 64 + 64, :]
            low = raw[half, a * 64 : a * 64 + 8, :]
            up = jnp.where(node == a, pltpu.roll(high, (a * 8 + 72) % 128, 1), up)
            down = jnp.where(node == a, pltpu.roll(low, a * 8, 1), down)
        b_send[0, half] = up
        b_send[1, half] = down

    steps = (1, -1)

    def face_copy(i):
        if i < 2:
            source, sink, target = a_send.at[i], a_recv.at[i], wrapped(steps[i], 0)
        else:
            source, sink, target = b_send.at[i - 2], b_recv.at[i - 2], wrapped(0, steps[i - 2])
        return pltpu.make_async_remote_copy(
            src_ref=source, dst_ref=sink,
            send_sem=face_send_sem.at[i], recv_sem=face_recv_sem.at[i],
            device_id=target, device_id_type=MESH,
        )

    def edge_copy(i, j):
        return pltpu.make_async_remote_copy(
            src_ref=b_send.at[j, 1 - i], dst_ref=edge_recv.at[j, i],
            send_sem=edge_send_sem.at[j, i], recv_sem=edge_recv_sem.at[j, i],
            device_id=wrapped(steps[i], steps[j]), device_id_type=MESH,
        )

    sends_a, sends_b = (g < grp_count - 1, g > 0), (d < dev_count - 1, d > 0)
    gets_a, gets_b = (g > 0, g < grp_count - 1), (d > 0, d < dev_count - 1)

    def clear(ref, i):
        ref[i] = jnp.zeros_like(ref[i])

    when(d > 0, lambda: pl.semaphore_wait(ready_sem, 1))
    for j in range(1, grp_count):
        group_copy(j).start()
    for j in range(2):
        for i in range(2):
            when(sends_a[i] & sends_b[j], lambda: edge_copy(i, j).start())
    for i in range(2):
        when(sends_a[i], lambda: face_copy(i).start())
        when(sends_b[i], lambda: face_copy(2 + i).start())

    lax.fori_loop(split, BATCHES, only_inner, 0)
    place(inner_rows[...], INNER_PAIRS)

    low_rows, high_rows = slice(0, 64), slice(448, 512)
    low = [raw[half, low_rows, :] for half in range(2)]
    high = [raw[half, high_rows, :] for half in range(2)]
    low_rolled = [pltpu.roll(x, 64, 1) for x in low]
    high_rolled = [pltpu.roll(x, 64, 1) for x in high]
    raw[0, low_rows, :] = low[0] + jnp.where(lower_half, 0.0, high_rolled[0])
    raw[1, low_rows, :] = low[1] + jnp.where(lower_half, high_rolled[0], high_rolled[1])
    raw[0, high_rows, :] = high[0] + jnp.where(lower_half, low_rolled[0], low_rolled[1])
    raw[1, high_rows, :] = high[1] + jnp.where(lower_half, low_rolled[1], 0.0)

    def from_below(high):
        return jnp.where(node == 0, 0.0, pltpu.roll(high, 8, 1))

    def from_above(low):
        return jnp.where(node == 7, 0.0, pltpu.roll(low, 120, 1))

    for half in range(2):
        for a in range(8):
            low_rows, high_rows = slice(a * 64, a * 64 + 8), slice(a * 64 + 56, a * 64 + 64)
            low, high = raw[half, low_rows, :], raw[half, high_rows, :]
            raw[half, low_rows, :] = low + from_below(high)
            raw[half, high_rows, :] = high + from_above(low)

    for i in range(2):
        when(gets_a[i], lambda: face_copy(i).wait_recv())
        when(jnp.logical_not(gets_a[i]), lambda: clear(a_recv, i))
    for i in range(2):
        got = a_recv[i]
        parts = [got, pltpu.roll(got, 64, 1)]
        if i == 0:
            got = jnp.where(lower_half, jnp.concatenate(parts, axis=0), 0.0)
        else:
            got = jnp.where(lower_half, 0.0, jnp.concatenate(parts[::-1], axis=0))
        start = i * 448
        raw[i, start : start + 8, :] += got[0:8] + from_below(got[56:64])
        raw[i, start + 8 : start + 56, :] += got[8:56]
        raw[i, start + 56 : start + 64, :] += got[56:64] + from_above(got[0:8])

    faces = []
    for j in range(2):
        when(gets_b[j], lambda: face_copy(2 + j).wait_recv())
        when(jnp.logical_not(gets_b[j]), lambda: clear(b_recv, j))
        for i in range(2):
            both = gets_a[i] & gets_b[j]
            when(both, lambda: edge_copy(i, j).wait_recv())
            when(jnp.logical_not(both), lambda: clear(edge_recv, (j, i)))
        first, second = b_recv[j, 0], b_recv[j, 1]
        up = [pltpu.roll(x, 8, 1) for x in (edge_recv[j, 0], first, second)]
        down = [pltpu.roll(x, 120, 1) for x in (first, second, edge_recv[j, 1])]
        face = []
        for half, own in enumerate((first, second)):
            from_low = jnp.where(lower_half, up[half], up[half + 1])
            from_high = jnp.where(lower_half, down[half], down[half + 1])
            face.append(
                own + jnp.where(node == 0, from_low, jnp.where(node == 7, from_high, 0.0))
            )
        faces.append(face)
    for half in range(2):
        for a in range(8):
            low_rows, high_rows = slice(a * 64, a * 64 + 8), slice(a * 64 + 56, a * 64 + 64)
            got_low = pltpu.roll(faces[0][half], (128 - a * 8) % 128, 1)
            got_high = pltpu.roll(faces[1][half], (56 - a * 8) % 128, 1)
            raw[half, low_rows, :] += jnp.where(node == 0, got_low, 0.0)
            raw[half, high_rows, :] += jnp.where(node == 7, got_high, 0.0)

    ez = lane % 8
    for half in range(2):
        for a in range(8):
            low_rows = pl.ds(a * 64, 8, stride=8)
            high_rows = pl.ds(a * 64 + 7, 8, stride=8)
            low, high = raw[half, low_rows, :], raw[half, high_rows, :]
            raw[half, low_rows, :] = low + jnp.where(ez > 0, pltpu.roll(high, 1, 1), 0.0)
            raw[half, high_rows, :] = high + jnp.where(ez < 7, pltpu.roll(low, 127, 1), 0.0)
        for part in range(4):
            rows = slice(part * 128, (part + 1) * 128)
            out[half * LANES : (half + 1) * LANES, rows] = raw[half, rows, :].T

    all_cost = group_send[...]
    for j in range(1, grp_count):
        group_copy(j).wait_recv()
        all_cost = all_cost + group_recv[j]
    cost[...] = all_cost

    for p in range(dev_count):
        when(p != d, lambda: data_copy(p, p).wait_send())
    for j in range(1, grp_count):
        group_copy(j).wait_send()
    for i in range(2):
        when(sends_a[i], lambda: face_copy(i).wait_send())
        when(sends_b[i], lambda: face_copy(2 + i).wait_send())
        for j in range(2):
            when(sends_a[i] & sends_b[j], lambda: edge_copy(i, j).wait_send())


def on_device(obs_coord, obs_resid, obs_weight, obs_dest, obs_send_slot, obs_elem, obs_slot):
    dev_count = lax.axis_size("dev")
    grp_count = lax.axis_size("grp")
    row_count = obs_resid.shape[0]
    obs_rows = row_count // LANES
    capacity = 2 * row_count // dev_count
    per_dest = capacity // LANES
    batch_rows = dev_count // BATCHES * per_dest
    vmem = pl.BlockSpec(memory_space=pltpu.VMEM)
    dma = pltpu.SemaphoreType.DMA
    regular = pltpu.SemaphoreType.REGULAR
    rows = [
        x.reshape(obs_rows, LANES)
        for x in (obs_resid, obs_weight, obs_dest, obs_send_slot, obs_elem)
    ]
    field, cost = pl.pallas_call(
        functools.partial(kernel, dev_count, grp_count, capacity),
        out_shape=(
            pltpu.VMEM((ELEM_DEV, 512), F32),
            pltpu.VMEM((1, LANES), F32),
        ),
        in_specs=[pl.BlockSpec(memory_space=pl.ANY)] * 6,
        out_specs=(vmem, vmem),
        scratch_shapes=[
            pltpu.VMEM((3, row_count), F32),
            pltpu.VMEM((obs_rows, LANES), F32),
            pltpu.VMEM((obs_rows, LANES), F32),
            pltpu.VMEM((obs_rows, LANES), jnp.int32),
            pltpu.VMEM((obs_rows, LANES), jnp.int32),
            pltpu.VMEM((obs_rows, LANES), jnp.int32),
            pltpu.VMEM((5, obs_rows, LANES), F32),
            pltpu.VMEM((dev_count, CHANNELS * per_dest + 1, LANES), F32),
            pltpu.VMEM((dev_count, CHANNELS * per_dest + 1, LANES), F32),
            pltpu.VMEM((1, LANES), F32),
            pltpu.VMEM((grp_count, 1, LANES), F32),
            pltpu.VMEM((BATCHES, 64, batch_rows, LANES), F32),
            pltpu.VMEM((BATCHES, 8 * batch_rows, LANES), F32),
            pltpu.VMEM((len(OUTER_PAIRS) * 8, ELEM_DEV), F32),
            pltpu.VMEM((len(INNER_PAIRS) * 8, ELEM_DEV), F32),
            pltpu.VMEM((2, 512, LANES), F32),
            pltpu.VMEM((2, 32, LANES), F32),
            pltpu.VMEM((2, 32, LANES), F32),
            pltpu.VMEM((2, 2, 8, LANES), F32),
            pltpu.VMEM((2, 2, 8, LANES), F32),
            pltpu.VMEM((2, 2, 8, LANES), F32),
            dma((dev_count,)),
            dma((dev_count,)),
            dma((grp_count,)),
            dma((grp_count,)),
            dma((4,)),
            dma((4,)),
            dma((2, 2)),
            dma((2, 2)),
            dma((6,)),
            regular((dev_count,)),
            regular,
            regular,
        ],
        compiler_params=pltpu.CompilerParams(collective_id=0, has_side_effects=True),
    )(obs_coord, *rows)
    return field.reshape(EX, EY, EZ, 512), cost[0, 0]


def solution(mesh):
    placed = (
        P(None, ("grp", "dev")),
        P(("grp", "dev")),
        P(("grp", "dev")),
        P(("grp", "dev")),
        P(("grp", "dev")),
        P(("grp", "dev")),
        P(("grp", "dev")),
    )
    return jax.shard_map(
        on_device,
        mesh=mesh,
        in_specs=placed,
        out_specs=(P("grp", "dev", None, None), P()),
        check_vma=False,
    )
```

```python
import functools
import math

import jax
import jax.numpy as jnp
from jax import lax
from jax.experimental import pallas as pl
from jax.experimental.pallas import tpu as pltpu
from jax.sharding import PartitionSpec as P

EX = 4
EY = 8
EZ = 8
ELEM_DEV = 256
LANES = 128
CHANNELS = 5
BATCHES = 4
MESH = pl.DeviceIdType.MESH
F32 = jnp.float32
BF16 = jnp.bfloat16
F8 = jnp.float8_e4m3fn

ANCHORS = [-math.cos(math.pi * k / 7) for k in range(8)]
OUTER_PAIRS = [(a, b) for a in (0, 7) for b in range(8)]
OUTER_PAIRS += [(a, b) for a in range(1, 7) for b in (0, 7)]
INNER_PAIRS = [(a, b) for a in range(1, 7) for b in range(1, 7)]
PAIRS = OUTER_PAIRS + INNER_PAIRS
COEFS = [
    1.0 / math.prod(ANCHORS[a] - ANCHORS[m] for m in range(8) if m != a) for a in range(8)
]


def basis_values(t):
    factors = [t - p for p in ANCHORS]
    prefix = [None] * 8
    suffix = [None] * 8
    for k in range(1, 8):
        prefix[k] = factors[k - 1] if k == 1 else prefix[k - 1] * factors[k - 1]
    for k in range(6, -1, -1):
        suffix[k] = factors[k + 1] if k == 6 else suffix[k + 1] * factors[k + 1]
    basis = []
    for a in range(8):
        if a == 0:
            product = suffix[0]
        elif a == 7:
            product = prefix[7]
        else:
            product = prefix[a] * suffix[a]
        basis.append(product * COEFS[a])
    return basis


def dot_nt(left, right):
    return lax.dot_general(left, right, (((1,), (1,)), ((), ())), preferred_element_type=F32)


def halves(row):
    value = jnp.broadcast_to(row, (16, LANES))
    first = value.astype(BF16)
    return first, (value - first.astype(F32)).astype(BF16)


def one_hot(row, ids):
    tile = jnp.broadcast_to(row, (ids[0].shape[0], LANES)).astype(BF16)
    return [jnp.where(part == tile, jnp.ones((), BF16), jnp.zeros((), BF16)) for part in ids]


def spread(hot, tiles):
    return jnp.concatenate([part * tile for tile in tiles for part in hot], axis=0)


def sublane_ids(count, step=16):
    ids = lax.broadcasted_iota(jnp.int32, (step, LANES), 0)
    return [(ids + step * i).astype(F32).astype(BF16) for i in range(count // step)]


def kernel(
    dev_count, grp_count, capacity,
    coord_in, resid_in, weight_in, dest_in, slot_in, elem_in,
    out, cost,
    coord, resid, weight, dest, slot, elem, terms, send, recv,
    group_send, group_recv,
    outer, third, face_rows, inner_rows, raw, a_send, a_recv, b_send, b_recv, edge_recv,
    send_sem, recv_sem, group_send_sem, group_recv_sem,
    face_send_sem, face_recv_sem, edge_send_sem, edge_recv_sem, load_sem,
    up_sem, head_sem, ready_sem,
):
    g = lax.axis_index("grp")
    d = lax.axis_index("dev")
    obs_rows = resid.shape[0]
    per_dest = capacity // LANES
    half_dev = dev_count // 2
    quarter_dev = half_dev // 2
    row_total = quarter_dev * per_dest
    batch = dev_count // BATCHES

    def when(condition, action):
        @pl.when(condition)
        def _():
            action()

    def wrapped(step_g, step_d):
        return (
            lax.rem(g + step_g + grp_count, grp_count),
            lax.rem(d + step_d + dev_count, dev_count),
        )

    loads = [
        pltpu.make_async_copy(source, sink, load_sem.at[i])
        for i, (source, sink) in enumerate(
            zip(
                (dest_in, slot_in, resid_in, weight_in, coord_in, elem_in),
                (dest, slot, resid, weight, coord, elem),
            )
        )
    ]
    for load in loads:
        load.start()

    barrier = pltpu.get_barrier_semaphore()
    def signal(semaphore, partner):
        pl.semaphore_signal(semaphore, inc=1, device_id=partner, device_id_type=MESH)

    heads = [wrapped(j, 0) for j in range(1, grp_count)]
    for p in range(dev_count):
        when(p > d, lambda: signal(barrier, (g, p)))
    for head in heads:
        when(d == 0, lambda: signal(barrier, head))
    pl.semaphore_wait(barrier, jnp.where(d == 0, len(heads), d))
    for p in range(dev_count):
        when(p < d, lambda: signal(up_sem.at[d], (g, p)))

    for load in loads:
        load.wait()

    cost_row = slice(CHANNELS * per_dest, CHANNELS * per_dest + 1)

    row_ids = sublane_ids(row_total)
    lane_ids = sublane_ids(2 * LANES, 32)
    once = jnp.minimum(d + 1, 1)

    def looped(body):
        def step(_, carry):
            body()
            return carry

        lax.fori_loop(0, once, step, 0)

    def set_terms():
        residual = resid[...]
        forcing = weight[...] * residual
        where = dest[...]
        which = slot[...]
        row = where % quarter_dev * per_dest + which // LANES
        for half in range(2):
            terms[half] = jnp.where(where // half_dev == half, row, -1).astype(F32)
        terms[2] = (where // quarter_dev % 2 * LANES + which % LANES).astype(F32)
        terms[3] = forcing
        terms[4] = elem[...].astype(F32)
        part = jnp.sum(forcing * residual, axis=0, keepdims=True)
        part = jnp.broadcast_to(0.5 * jnp.sum(part, axis=1, keepdims=True), (1, LANES))
        for p in range(dev_count):
            send[p, cost_row, :] = part

    def pack(half):
        left, right = [], []
        for r in range(obs_rows):
            columns = slice(r * LANES, (r + 1) * LANES)
            values = [halves(coord[c : c + 1, columns]) for c in range(3)]
            values.append(halves(terms[3, r : r + 1, :]))
            tiles = [high for high, _ in values]
            tiles.append(halves(terms[4, r : r + 1, :])[0])
            tiles += [low for _, low in values]
            left.append(spread(one_hot(terms[half, r : r + 1, :], row_ids), tiles))
            hot = one_hot(terms[2, r : r + 1, :], lane_ids)
            right.append(jnp.concatenate([part.astype(F8) for part in hot], axis=0))
        packed = dot_nt(jnp.concatenate(left, axis=1), jnp.concatenate(right, axis=1))
        for q in range(half_dev):
            lanes = slice(q // quarter_dev * LANES, (q // quarter_dev + 1) * LANES)
            for c in range(CHANNELS):
                start = c * row_total + q % quarter_dev * per_dest
                rows = packed[start : start + per_dest, lanes]
                if c < 4:
                    start = (c + CHANNELS) * row_total + q % quarter_dev * per_dest
                    rows = rows + packed[start : start + per_dest, lanes]
                send[half * half_dev + q, c * per_dest : (c + 1) * per_dest, :] = rows

    def data_copy(p, source):
        return pltpu.make_async_remote_copy(
            src_ref=send.at[p], dst_ref=recv.at[source],
            send_sem=send_sem.at[p], recv_sem=recv_sem.at[source],
            device_id=(g, p), device_id_type=MESH,
        )

    def group_copy(j):
        return pltpu.make_async_remote_copy(
            src_ref=group_send, dst_ref=group_recv.at[j],
            send_sem=group_send_sem.at[j], recv_sem=group_recv_sem.at[j],
            device_id=wrapped(j, 0), device_id_type=MESH,
        )

    own = d // batch

    def send_to(p):
        when(p > d, lambda: pl.semaphore_wait(up_sem.at[p], 1))
        data_copy(p, d).start()

    def pack_first():
        set_terms()
        pack(0)

    looped(pack_first)
    for p in range(half_dev):
        when(p < d, lambda: send_to(p))
    looped(lambda: pack(1))
    for p in range(half_dev, dev_count):
        when(p < d, lambda: send_to(p))
    for i in range(batch):
        when(own * batch + i > d, lambda: send_to(own * batch + i))

    def send_up(x):
        for i in range(batch):
            when(x < BATCHES, lambda: send_to(x * batch + i))

    send_up(own + 1)
    recv[d] = send[d]

    elem_ids = sublane_ids(ELEM_DEV, 32)
    rows = batch * per_dest

    def prepare(x, t):
        def channel(c):
            start = c * per_dest
            parts = [recv[x * batch + i, start : start + per_dest, :] for i in range(batch)]
            return jnp.concatenate(parts, axis=0)

        weighted = [first * channel(3) for first in basis_values(channel(0))]
        second = basis_values(channel(1))
        for c, value in enumerate(basis_values(channel(2))):
            third[t, c * rows : (c + 1) * rows, :] = value
        for i, (a, b) in enumerate(PAIRS):
            outer[t, i] = weighted[a] * second[b]

    def pair_sums(x, t, groups):
        left, right = [], []
        for h in range(rows):
            w = third[t, pl.ds(h, 8, stride=rows), :]
            pieces = []
            for start, stop in groups:
                highs, lows = [], []
                for i in range(start, stop, 2):
                    value = jnp.concatenate([outer[t, k, h : h + 1, :] * w for k in (i, i + 1)], axis=0)
                    high = value.astype(BF16)
                    highs.append(high)
                    lows.append((value - high.astype(F32)).astype(BF16))
                pieces += highs + lows
            left.append(jnp.concatenate(pieces, axis=0))
            start = 4 * per_dest + h % per_dest
            owner = recv[x * batch + h // per_dest, start : start + 1, :]
            hot = one_hot(owner, elem_ids)
            right.append(jnp.concatenate([part.astype(F8) for part in hot], axis=0))
        total = dot_nt(jnp.concatenate(left, axis=1), jnp.concatenate(right, axis=1))
        sums, row = [], 0
        for start, stop in groups:
            count = (stop - start) * 8
            sums.append(total[row : row + count] + total[row + count : row + 2 * count])
            row += 2 * count
        return sums

    faces, inners = (0, len(OUTER_PAIRS)), (len(OUTER_PAIRS), len(PAIRS))

    def arrive(source):
        data_copy(source, source).wait_recv()

    for i in range(batch):
        when(own * batch + i != d, lambda: arrive(own * batch + i))

    def first_sums():
        prepare(own, 0)
        face_rows[...], inner_rows[...] = pair_sums(own, 0, (faces, inners))

    looped(first_sums)

    for j in range(2, BATCHES):
        send_up(own + j)
    for head in heads:
        when(d == 0, lambda: signal(head_sem, head))

    def batch_of(t):
        early = own < BATCHES // 2
        turn = jnp.where(early, own, BATCHES - 1 - own)
        x = t - 1 + (t > turn).astype(jnp.int32)
        return jnp.where(early, x, BATCHES - 1 - x)

    def from_batch(t):
        x = batch_of(t)
        for i in range(batch):
            arrive(x * batch + i)
        prepare(x, t)
        return x

    def tell_ready():
        pl.semaphore_wait(head_sem, len(heads))
        for p in range(1, dev_count):
            signal(ready_sem, (g, p))

    def only_faces(t, carry):
        face_rows[...] += pair_sums(from_batch(t), t, (faces,))[0]
        when((d == 0) & (t == 1), tell_ready)
        return carry

    def only_inner(t, carry):
        inner_rows[...] += pair_sums(batch_of(t), t, (inners,))[0]
        return carry

    lax.fori_loop(1, BATCHES - 1, only_faces, 0)
    last = from_batch(BATCHES - 1)
    group_cost = recv[0, cost_row, :]
    for i in range(1, dev_count):
        group_cost = group_cost + recv[i, cost_row, :]
    group_send[...] = group_cost
    when(d > 0, lambda: pl.semaphore_wait(ready_sem, 1))
    for j in range(1, grp_count):
        group_copy(j).start()

    def place(value, pairs):
        for i, (a, b) in enumerate(pairs):
            start = a * 64 + b * 8
            for half in range(2):
                lanes = slice(half * LANES, (half + 1) * LANES)
                raw[half, start : start + 8, :] = value[i * 8 : i * 8 + 8, lanes]

    def last_faces():
        place(face_rows[...] + pair_sums(last, BATCHES - 1, (faces,))[0], OUTER_PAIRS)

    looped(last_faces)

    lane = lax.broadcasted_iota(jnp.int32, (1, LANES), 1)
    lower_half = lane < 64
    node = (lane // 8) % 8
    block = raw[1, 448:512, :]
    a_send[0] = jnp.where(lower_half, pltpu.roll(block[0:32], 64, 1), block[32:64])
    block = raw[0, 0:64, :]
    a_send[1] = jnp.where(lower_half, block[0:32], pltpu.roll(block[32:64], 64, 1))
    for half in range(2):
        up = pltpu.roll(raw[half, 56:64, :], 72, 1)
        down = raw[half, 0:8, :]
        for a in range(1, 8):
            high = raw[half, a * 64 + 56 : a * 64 + 64, :]
            low = raw[half, a * 64 : a * 64 + 8, :]
            up = jnp.where(node == a, pltpu.roll(high, (a * 8 + 72) % 128, 1), up)
            down = jnp.where(node == a, pltpu.roll(low, a * 8, 1), down)
        b_send[0, half] = up
        b_send[1, half] = down

    steps = (1, -1)

    def face_copy(i):
        if i < 2:
            source, sink, target = a_send.at[i], a_recv.at[i], wrapped(steps[i], 0)
        else:
            source, sink, target = b_send.at[i - 2], b_recv.at[i - 2], wrapped(0, steps[i - 2])
        return pltpu.make_async_remote_copy(
            src_ref=source, dst_ref=sink,
            send_sem=face_send_sem.at[i], recv_sem=face_recv_sem.at[i],
            device_id=target, device_id_type=MESH,
        )

    def edge_copy(i, j):
        return pltpu.make_async_remote_copy(
            src_ref=b_send.at[j, 1 - i], dst_ref=edge_recv.at[j, i],
            send_sem=edge_send_sem.at[j, i], recv_sem=edge_recv_sem.at[j, i],
            device_id=wrapped(steps[i], steps[j]), device_id_type=MESH,
        )

    sends_a, sends_b = (g < grp_count - 1, g > 0), (d < dev_count - 1, d > 0)
    gets_a, gets_b = (g > 0, g < grp_count - 1), (d > 0, d < dev_count - 1)

    def clear(ref, i):
        ref[i] = jnp.zeros_like(ref[i])

    for i in (1, 0):
        for j in range(2):
            when(sends_a[i] & sends_b[j], lambda: edge_copy(i, j).start())
    for i in (1, 0):
        when(sends_a[i], lambda: face_copy(i).start())
        when(sends_b[i], lambda: face_copy(2 + i).start())

    lax.fori_loop(1, BATCHES, only_inner, 0)
    place(inner_rows[...], INNER_PAIRS)

    low_rows, high_rows = slice(0, 64), slice(448, 512)
    low = [raw[half, low_rows, :] for half in range(2)]
    high = [raw[half, high_rows, :] for half in range(2)]
    low_rolled = [pltpu.roll(x, 64, 1) for x in low]
    high_rolled = [pltpu.roll(x, 64, 1) for x in high]
    raw[0, low_rows, :] = low[0] + jnp.where(lower_half, 0.0, high_rolled[0])
    raw[1, low_rows, :] = low[1] + jnp.where(lower_half, high_rolled[0], high_rolled[1])
    raw[0, high_rows, :] = high[0] + jnp.where(lower_half, low_rolled[0], low_rolled[1])
    raw[1, high_rows, :] = high[1] + jnp.where(lower_half, low_rolled[1], 0.0)

    def from_below(high):
        return jnp.where(node == 0, 0.0, pltpu.roll(high, 8, 1))

    def from_above(low):
        return jnp.where(node == 7, 0.0, pltpu.roll(low, 120, 1))

    for half in range(2):
        for a in range(8):
            low_rows, high_rows = slice(a * 64, a * 64 + 8), slice(a * 64 + 56, a * 64 + 64)
            low, high = raw[half, low_rows, :], raw[half, high_rows, :]
            raw[half, low_rows, :] = low + from_below(high)
            raw[half, high_rows, :] = high + from_above(low)

    for i in range(2):
        when(gets_a[i], lambda: face_copy(i).wait_recv())
        when(jnp.logical_not(gets_a[i]), lambda: clear(a_recv, i))
    for i in range(2):
        got = a_recv[i]
        far = pltpu.roll(got, 64, 1)
        start = i * 448
        if i == 0:
            keep, low, high = lower_half, got[0:8], pltpu.roll(got[24:32], 72, 1)
            low = pltpu.roll(low, 120, 1)
            got = jnp.concatenate([got, far], axis=0)
        else:
            keep, low, high = jnp.logical_not(lower_half), pltpu.roll(got[0:8], 56, 1), got[24:32]
            high = pltpu.roll(high, 8, 1)
            got = jnp.concatenate([far, got], axis=0)
        got = jnp.where(keep, got, 0.0)
        raw[i, start : start + 8, :] += got[0:8] + jnp.where(keep & (node > 0), high, 0.0)
        raw[i, start + 8 : start + 56, :] += got[8:56]
        raw[i, start + 56 : start + 64, :] += got[56:64] + jnp.where(keep & (node < 7), low, 0.0)

    for j in range(2):
        when(gets_b[j], lambda: face_copy(2 + j).wait_recv())
        when(jnp.logical_not(gets_b[j]), lambda: clear(b_recv, j))
        for i in range(2):
            both = gets_a[i] & gets_b[j]
            when(both, lambda: edge_copy(i, j).wait_recv())
            when(jnp.logical_not(both), lambda: clear(edge_recv, (j, i)))
    for j in range(2):
        mine = [b_recv[j, 0], b_recv[j, 1]]
        up = [pltpu.roll(x, (8, 64)[j], 1) for x in (edge_recv[j, 0], *mine)]
        down = [pltpu.roll(x, (64, 120)[j], 1) for x in (*mine, edge_recv[j, 1])]
        for half in range(2):
            for a in range(8):
                got = pltpu.roll(mine[half], (56 * j - a * 8) % 128, 1)
                if a == 0:
                    got = got + jnp.where(lower_half, up[half], up[half + 1])
                if a == 7:
                    got = got + jnp.where(lower_half, down[half], down[half + 1])
                start = a * 64 + 56 * j
                raw[half, start : start + 8, :] += jnp.where(node == 7 * j, got, 0.0)

    ez = lane % 8
    for half in range(2):
        for a in range(8):
            low_rows = pl.ds(a * 64, 8, stride=8)
            high_rows = pl.ds(a * 64 + 7, 8, stride=8)
            low, high = raw[half, low_rows, :], raw[half, high_rows, :]
            raw[half, low_rows, :] = low + jnp.where(ez > 0, pltpu.roll(high, 1, 1), 0.0)
            raw[half, high_rows, :] = high + jnp.where(ez < 7, pltpu.roll(low, 127, 1), 0.0)
        for part in range(4):
            rows = slice(part * 128, (part + 1) * 128)
            out[half * LANES : (half + 1) * LANES, rows] = raw[half, rows, :].T

    all_cost = group_send[...]
    for j in range(1, grp_count):
        group_copy(j).wait_recv()
        all_cost = all_cost + group_recv[j]
    cost[...] = all_cost

    for p in range(dev_count):
        when(p != d, lambda: data_copy(p, p).wait_send())
    for j in range(1, grp_count):
        group_copy(j).wait_send()
    for i in range(2):
        when(sends_a[i], lambda: face_copy(i).wait_send())
        when(sends_b[i], lambda: face_copy(2 + i).wait_send())
        for j in range(2):
            when(sends_a[i] & sends_b[j], lambda: edge_copy(i, j).wait_send())


def on_device(obs_coord, obs_resid, obs_weight, obs_dest, obs_send_slot, obs_elem, obs_slot):
    dev_count = lax.axis_size("dev")
    grp_count = lax.axis_size("grp")
    row_count = obs_resid.shape[0]
    obs_rows = row_count // LANES
    capacity = 2 * row_count // dev_count
    per_dest = capacity // LANES
    batch_rows = dev_count // BATCHES * per_dest
    vmem = pl.BlockSpec(memory_space=pltpu.VMEM)
    dma = pltpu.SemaphoreType.DMA
    regular = pltpu.SemaphoreType.REGULAR
    rows = [
        x.reshape(obs_rows, LANES)
        for x in (obs_resid, obs_weight, obs_dest, obs_send_slot, obs_elem)
    ]
    field, cost = pl.pallas_call(
        functools.partial(kernel, dev_count, grp_count, capacity),
        out_shape=(
            pltpu.VMEM((ELEM_DEV, 512), F32),
            pltpu.VMEM((1, LANES), F32),
        ),
        in_specs=[pl.BlockSpec(memory_space=pl.ANY)] * 6,
        out_specs=(vmem, vmem),
        scratch_shapes=[
            pltpu.VMEM((3, row_count), F32),
            pltpu.VMEM((obs_rows, LANES), F32),
            pltpu.VMEM((obs_rows, LANES), F32),
            pltpu.VMEM((obs_rows, LANES), jnp.int32),
            pltpu.VMEM((obs_rows, LANES), jnp.int32),
            pltpu.VMEM((obs_rows, LANES), jnp.int32),
            pltpu.VMEM((5, obs_rows, LANES), F32),
            pltpu.VMEM((dev_count, CHANNELS * per_dest + 1, LANES), F32),
            pltpu.VMEM((dev_count, CHANNELS * per_dest + 1, LANES), F32),
            pltpu.VMEM((1, LANES), F32),
            pltpu.VMEM((grp_count, 1, LANES), F32),
            pltpu.VMEM((BATCHES, 64, batch_rows, LANES), F32),
            pltpu.VMEM((BATCHES, 8 * batch_rows, LANES), F32),
            pltpu.VMEM((len(OUTER_PAIRS) * 8, ELEM_DEV), F32),
            pltpu.VMEM((len(INNER_PAIRS) * 8, ELEM_DEV), F32),
            pltpu.VMEM((2, 512, LANES), F32),
            pltpu.VMEM((2, 32, LANES), F32),
            pltpu.VMEM((2, 32, LANES), F32),
            pltpu.VMEM((2, 2, 8, LANES), F32),
            pltpu.VMEM((2, 2, 8, LANES), F32),
            pltpu.VMEM((2, 2, 8, LANES), F32),
            dma((dev_count,)),
            dma((dev_count,)),
            dma((grp_count,)),
            dma((grp_count,)),
            dma((4,)),
            dma((4,)),
            dma((2, 2)),
            dma((2, 2)),
            dma((6,)),
            regular((dev_count,)),
            regular,
            regular,
        ],
        compiler_params=pltpu.CompilerParams(collective_id=0, has_side_effects=True),
    )(obs_coord, *rows)
    return field.reshape(EX, EY, EZ, 512), cost[0, 0]


def solution(mesh):
    placed = (
        P(None, ("grp", "dev")),
        P(("grp", "dev")),
        P(("grp", "dev")),
        P(("grp", "dev")),
        P(("grp", "dev")),
        P(("grp", "dev")),
        P(("grp", "dev")),
    )
    return jax.shard_map(
        on_device,
        mesh=mesh,
        in_specs=placed,
        out_specs=(P("grp", "dev", None, None), P()),
        check_vma=False,
    )
```

```python
import functools
import math

import jax
import jax.numpy as jnp
from jax import lax
from jax.experimental import pallas as pl
from jax.experimental.pallas import tpu as pltpu
from jax.sharding import PartitionSpec as P

EX = 4
EY = 8
EZ = 8
ELEM_DEV = 256
LANES = 128
CHANNELS = 5
BATCHES = 4
MESH = pl.DeviceIdType.MESH
F32 = jnp.float32
BF16 = jnp.bfloat16
F8 = jnp.float8_e4m3fn

ANCHORS = [-math.cos(math.pi * k / 7) for k in range(8)]
OUTER_PAIRS = [(a, b) for a in (0, 7) for b in range(8)]
OUTER_PAIRS += [(a, b) for a in range(1, 7) for b in (0, 7)]
INNER_PAIRS = [(a, b) for a in range(1, 7) for b in range(1, 7)]
PAIRS = OUTER_PAIRS + INNER_PAIRS
COEFS = [
    1.0 / math.prod(ANCHORS[a] - ANCHORS[m] for m in range(8) if m != a) for a in range(8)
]


def basis_values(t):
    factors = [t - p for p in ANCHORS]
    prefix = [None] * 8
    suffix = [None] * 8
    for k in range(1, 8):
        prefix[k] = factors[k - 1] if k == 1 else prefix[k - 1] * factors[k - 1]
    for k in range(6, -1, -1):
        suffix[k] = factors[k + 1] if k == 6 else suffix[k + 1] * factors[k + 1]
    basis = []
    for a in range(8):
        if a == 0:
            product = suffix[0]
        elif a == 7:
            product = prefix[7]
        else:
            product = prefix[a] * suffix[a]
        basis.append(product * COEFS[a])
    return basis


def dot_nt(left, right):
    return lax.dot_general(left, right, (((1,), (1,)), ((), ())), preferred_element_type=F32)


def halves(row):
    value = jnp.broadcast_to(row, (16, LANES))
    first = value.astype(BF16)
    return first, (value - first.astype(F32)).astype(BF16)


def one_hot(row, ids):
    tile = jnp.broadcast_to(row, (ids[0].shape[0], LANES)).astype(BF16)
    return [jnp.where(part == tile, jnp.ones((), BF16), jnp.zeros((), BF16)) for part in ids]


def spread(hot, tiles):
    return jnp.concatenate([part * tile for tile in tiles for part in hot], axis=0)


def sublane_ids(count, step=16):
    ids = lax.broadcasted_iota(jnp.int32, (step, LANES), 0)
    return [(ids + step * i).astype(F32).astype(BF16) for i in range(count // step)]


def kernel(
    dev_count, grp_count, capacity,
    coord_in, resid_in, weight_in, dest_in, slot_in, elem_in,
    out, cost,
    coord, resid, weight, dest, slot, elem, terms, send, recv,
    group_send, group_recv,
    outer, third, face_rows, inner_rows, raw, a_send, a_recv, b_send, b_recv, edge_recv,
    send_sem, recv_sem, group_send_sem, group_recv_sem,
    face_send_sem, face_recv_sem, edge_send_sem, edge_recv_sem,
    up_sem, head_sem, ready_sem,
):
    g = lax.axis_index("grp")
    d = lax.axis_index("dev")
    obs_rows = resid.shape[0]
    per_dest = capacity // LANES
    half_dev = dev_count // 2
    quarter_dev = half_dev // 2
    row_total = quarter_dev * per_dest
    batch = dev_count // BATCHES

    def when(condition, action):
        @pl.when(condition)
        def _():
            action()

    def wrapped(step_g, step_d):
        return (
            lax.rem(g + step_g + grp_count, grp_count),
            lax.rem(d + step_d + dev_count, dev_count),
        )

    loads = [
        pltpu.make_async_copy(source, sink, send_sem.at[i])
        for i, (source, sink) in enumerate(
            zip(
                (dest_in, slot_in, resid_in, weight_in, coord_in, elem_in),
                (dest, slot, resid, weight, coord, elem),
            )
        )
    ]
    for load in loads:
        load.start()

    barrier = pltpu.get_barrier_semaphore()
    def signal(semaphore, partner):
        pl.semaphore_signal(semaphore, inc=1, device_id=partner, device_id_type=MESH)

    heads = [wrapped(j, 0) for j in range(1, grp_count)]
    for p in range(dev_count):
        when(p > d, lambda: signal(barrier, (g, p)))
    for head in heads:
        when(d == 0, lambda: signal(barrier, head))
    pl.semaphore_wait(barrier, jnp.where(d == 0, len(heads), d))
    for p in range(dev_count):
        when(p < d, lambda: signal(up_sem.at[d], (g, p)))

    for load in loads:
        load.wait()

    cost_row = slice(CHANNELS * per_dest, CHANNELS * per_dest + 1)

    row_ids = sublane_ids(row_total)
    lane_ids = sublane_ids(2 * LANES, 32)
    once = jnp.minimum(d + 1, 1)

    def looped(body):
        def step(_, carry):
            body()
            return carry

        lax.fori_loop(0, once, step, 0)

    def set_terms():
        residual = resid[...]
        forcing = weight[...] * residual
        where = dest[...]
        which = slot[...]
        row = where % quarter_dev * per_dest + which // LANES
        for half in range(2):
            terms[half] = jnp.where(where // half_dev == half, row, -1).astype(F32)
        terms[2] = (where // quarter_dev % 2 * LANES + which % LANES).astype(F32)
        terms[3] = forcing
        terms[4] = elem[...].astype(F32)
        part = jnp.sum(forcing * residual, axis=0, keepdims=True)
        part = jnp.broadcast_to(0.5 * jnp.sum(part, axis=1, keepdims=True), (1, LANES))
        for p in range(dev_count):
            send[p, cost_row, :] = part

    def pack(half):
        left, right = [], []
        for r in range(obs_rows):
            columns = slice(r * LANES, (r + 1) * LANES)
            values = [halves(coord[c : c + 1, columns]) for c in range(3)]
            values.append(halves(terms[3, r : r + 1, :]))
            tiles = [high for high, _ in values]
            tiles.append(halves(terms[4, r : r + 1, :])[0])
            tiles += [low for _, low in values]
            left.append(spread(one_hot(terms[half, r : r + 1, :], row_ids), tiles))
            hot = one_hot(terms[2, r : r + 1, :], lane_ids)
            right.append(jnp.concatenate([part.astype(F8) for part in hot], axis=0))
        packed = dot_nt(jnp.concatenate(left, axis=1), jnp.concatenate(right, axis=1))
        for q in range(half_dev):
            lanes = slice(q // quarter_dev * LANES, (q // quarter_dev + 1) * LANES)
            for c in range(CHANNELS):
                start = c * row_total + q % quarter_dev * per_dest
                rows = packed[start : start + per_dest, lanes]
                if c < 4:
                    start = (c + CHANNELS) * row_total + q % quarter_dev * per_dest
                    rows = rows + packed[start : start + per_dest, lanes]
                send[half * half_dev + q, c * per_dest : (c + 1) * per_dest, :] = rows

    def data_copy(p, source):
        return pltpu.make_async_remote_copy(
            src_ref=send.at[p], dst_ref=recv.at[source],
            send_sem=send_sem.at[p], recv_sem=recv_sem.at[source],
            device_id=(g, p), device_id_type=MESH,
        )

    def group_copy(j):
        return pltpu.make_async_remote_copy(
            src_ref=group_send, dst_ref=group_recv.at[j],
            send_sem=group_send_sem.at[j], recv_sem=group_recv_sem.at[j],
            device_id=wrapped(j, 0), device_id_type=MESH,
        )

    own = d // batch

    def send_to(p):
        when(p > d, lambda: pl.semaphore_wait(up_sem.at[p], 1))
        data_copy(p, d).start()

    def pack_first():
        set_terms()
        pack(0)

    looped(pack_first)
    for p in range(half_dev):
        when(p < d, lambda: send_to(p))
    looped(lambda: pack(1))
    for p in range(half_dev, dev_count):
        when(p < d, lambda: send_to(p))
    for i in range(batch):
        when(own * batch + i > d, lambda: send_to(own * batch + i))

    def send_up(x):
        for i in range(batch):
            when(x < BATCHES, lambda: send_to(x * batch + i))

    send_up(own + 1)
    recv[d] = send[d]

    elem_ids = sublane_ids(ELEM_DEV, 32)
    rows = batch * per_dest

    def prepare(x, t, begin=0, end=batch):
        def channel(c):
            start = c * per_dest
            parts = [recv[x * batch + i, start : start + per_dest, :] for i in range(begin, end)]
            return jnp.concatenate(parts, axis=0)

        first, last = begin * per_dest, end * per_dest
        weighted = [value * channel(3) for value in basis_values(channel(0))]
        second = basis_values(channel(1))
        for c, value in enumerate(basis_values(channel(2))):
            third[t, c * rows + first : c * rows + last, :] = value
        for i, (a, b) in enumerate(PAIRS):
            outer[t, i, first:last] = weighted[a] * second[b]

    def pair_sums(x, t, groups, begin=0, end=batch):
        left, right = [], []
        for h in range(begin * per_dest, end * per_dest):
            w = third[t, pl.ds(h, 8, stride=rows), :]
            pieces = []
            for start, stop in groups:
                highs, lows = [], []
                for i in range(start, stop, 2):
                    value = jnp.concatenate([outer[t, k, h : h + 1, :] * w for k in (i, i + 1)], axis=0)
                    high = value.astype(BF16)
                    highs.append(high)
                    lows.append((value - high.astype(F32)).astype(BF16))
                pieces += highs + lows
            left.append(jnp.concatenate(pieces, axis=0))
            start = 4 * per_dest + h % per_dest
            owner = recv[x * batch + h // per_dest, start : start + 1, :]
            hot = one_hot(owner, elem_ids)
            right.append(jnp.concatenate([part.astype(F8) for part in hot], axis=0))
        total = dot_nt(jnp.concatenate(left, axis=1), jnp.concatenate(right, axis=1))
        sums, row = [], 0
        for start, stop in groups:
            count = (stop - start) * 8
            sums.append(total[row : row + count] + total[row + count : row + 2 * count])
            row += 2 * count
        return sums

    faces, inners = (0, len(OUTER_PAIRS)), (len(OUTER_PAIRS), len(PAIRS))

    def arrive(source):
        data_copy(source, source).wait_recv()

    for i in range(batch):
        when(own * batch + i != d, lambda: arrive(own * batch + i))

    def first_sums():
        prepare(own, 0)
        face_rows[...], inner_rows[...] = pair_sums(own, 0, (faces, inners))

    looped(first_sums)

    for j in range(2, BATCHES):
        send_up(own + j)
    for head in heads:
        when(d == 0, lambda: signal(head_sem, head))

    def batch_of(t):
        early = own < BATCHES // 2
        turn = jnp.where(early, own, BATCHES - 1 - own)
        x = t - 1 + (t > turn).astype(jnp.int32)
        return jnp.where(early, x, BATCHES - 1 - x)

    def from_batch(t):
        x = batch_of(t)
        for i in range(batch):
            arrive(x * batch + i)
        prepare(x, t)
        return x

    def tell_ready():
        pl.semaphore_wait(head_sem, len(heads))
        for p in range(1, dev_count):
            signal(ready_sem, (g, p))

    def only_faces(t, carry):
        face_rows[...] += pair_sums(from_batch(t), t, (faces,))[0]
        when((d == 0) & (t == 1), tell_ready)
        return carry

    def only_inner(t, carry):
        inner_rows[...] += pair_sums(batch_of(t), t, (inners,))[0]
        return carry

    lax.fori_loop(1, BATCHES - 1, only_faces, 0)
    last = from_batch(BATCHES - 1)
    group_cost = recv[0, cost_row, :]
    for i in range(1, dev_count):
        group_cost = group_cost + recv[i, cost_row, :]
    group_send[...] = group_cost
    when(d > 0, lambda: pl.semaphore_wait(ready_sem, 1))
    for j in range(1, grp_count):
        group_copy(j).start()

    def place(value, pairs):
        for i, (a, b) in enumerate(pairs):
            start = a * 64 + b * 8
            for half in range(2):
                lanes = slice(half * LANES, (half + 1) * LANES)
                raw[half, start : start + 8, :] = value[i * 8 : i * 8 + 8, lanes]

    def last_faces():
        place(face_rows[...] + pair_sums(last, BATCHES - 1, (faces,))[0], OUTER_PAIRS)

    looped(last_faces)

    lane = lax.broadcasted_iota(jnp.int32, (1, LANES), 1)
    lower_half = lane < 64
    node = (lane // 8) % 8
    block = raw[1, 448:512, :]
    a_send[0] = jnp.where(lower_half, pltpu.roll(block[0:32], 64, 1), block[32:64])
    block = raw[0, 0:64, :]
    a_send[1] = jnp.where(lower_half, block[0:32], pltpu.roll(block[32:64], 64, 1))
    for half in range(2):
        up = pltpu.roll(raw[half, 56:64, :], 72, 1)
        down = raw[half, 0:8, :]
        for a in range(1, 8):
            high = raw[half, a * 64 + 56 : a * 64 + 64, :]
            low = raw[half, a * 64 : a * 64 + 8, :]
            up = jnp.where(node == a, pltpu.roll(high, (a * 8 + 72) % 128, 1), up)
            down = jnp.where(node == a, pltpu.roll(low, a * 8, 1), down)
        b_send[0, half] = up
        b_send[1, half] = down

    steps = (1, -1)

    def face_copy(i):
        if i < 2:
            source, sink, target = a_send.at[i], a_recv.at[i], wrapped(steps[i], 0)
        else:
            source, sink, target = b_send.at[i - 2], b_recv.at[i - 2], wrapped(0, steps[i - 2])
        return pltpu.make_async_remote_copy(
            src_ref=source, dst_ref=sink,
            send_sem=face_send_sem.at[i], recv_sem=face_recv_sem.at[i],
            device_id=target, device_id_type=MESH,
        )

    def edge_copy(i, j):
        return pltpu.make_async_remote_copy(
            src_ref=b_send.at[j, 1 - i], dst_ref=edge_recv.at[j, i],
            send_sem=edge_send_sem.at[j, i], recv_sem=edge_recv_sem.at[j, i],
            device_id=wrapped(steps[i], steps[j]), device_id_type=MESH,
        )

    sends_a, sends_b = (g < grp_count - 1, g > 0), (d < dev_count - 1, d > 0)
    gets_a, gets_b = (g > 0, g < grp_count - 1), (d > 0, d < dev_count - 1)

    def clear(ref, i):
        ref[i] = jnp.zeros_like(ref[i])

    for i in (1, 0):
        for j in range(2):
            when(sends_a[i] & sends_b[j], lambda: edge_copy(i, j).start())
    for i in (1, 0):
        when(sends_a[i], lambda: face_copy(i).start())
        when(sends_b[i], lambda: face_copy(2 + i).start())

    lax.fori_loop(1, BATCHES, only_inner, 0)
    place(inner_rows[...], INNER_PAIRS)

    low_rows, high_rows = slice(0, 64), slice(448, 512)
    low = [raw[half, low_rows, :] for half in range(2)]
    high = [raw[half, high_rows, :] for half in range(2)]
    low_rolled = [pltpu.roll(x, 64, 1) for x in low]
    high_rolled = [pltpu.roll(x, 64, 1) for x in high]
    raw[0, low_rows, :] = low[0] + jnp.where(lower_half, 0.0, high_rolled[0])
    raw[1, low_rows, :] = low[1] + jnp.where(lower_half, high_rolled[0], high_rolled[1])
    raw[0, high_rows, :] = high[0] + jnp.where(lower_half, low_rolled[0], low_rolled[1])
    raw[1, high_rows, :] = high[1] + jnp.where(lower_half, low_rolled[1], 0.0)

    def from_below(high):
        return jnp.where(node == 0, 0.0, pltpu.roll(high, 8, 1))

    def from_above(low):
        return jnp.where(node == 7, 0.0, pltpu.roll(low, 120, 1))

    for half in range(2):
        for a in range(8):
            low_rows, high_rows = slice(a * 64, a * 64 + 8), slice(a * 64 + 56, a * 64 + 64)
            low, high = raw[half, low_rows, :], raw[half, high_rows, :]
            raw[half, low_rows, :] = low + from_below(high)
            raw[half, high_rows, :] = high + from_above(low)

    all_cost = group_send[...]
    for j in range(1, grp_count):
        group_copy(j).wait_recv()
        all_cost = all_cost + group_recv[j]
    cost[...] = all_cost

    for p in range(dev_count):
        when(p != d, lambda: data_copy(p, p).wait_send())
    for j in range(1, grp_count):
        group_copy(j).wait_send()
    for i in range(2):
        when(sends_a[i], lambda: face_copy(i).wait_send())
        when(sends_b[i], lambda: face_copy(2 + i).wait_send())
        for j in range(2):
            when(sends_a[i] & sends_b[j], lambda: edge_copy(i, j).wait_send())

    for i in range(2):
        when(gets_a[i], lambda: face_copy(i).wait_recv())
        when(jnp.logical_not(gets_a[i]), lambda: clear(a_recv, i))
    for i in range(2):
        got = a_recv[i]
        far = pltpu.roll(got, 64, 1)
        start = i * 448
        if i == 0:
            keep, low, high = lower_half, got[0:8], pltpu.roll(got[24:32], 72, 1)
            low = pltpu.roll(low, 120, 1)
            got = jnp.concatenate([got, far], axis=0)
        else:
            keep, low, high = jnp.logical_not(lower_half), pltpu.roll(got[0:8], 56, 1), got[24:32]
            high = pltpu.roll(high, 8, 1)
            got = jnp.concatenate([far, got], axis=0)
        got = jnp.where(keep, got, 0.0)
        raw[i, start : start + 8, :] += got[0:8] + jnp.where(keep & (node > 0), high, 0.0)
        raw[i, start + 8 : start + 56, :] += got[8:56]
        raw[i, start + 56 : start + 64, :] += got[56:64] + jnp.where(keep & (node < 7), low, 0.0)

    for j in range(2):
        when(gets_b[j], lambda: face_copy(2 + j).wait_recv())
        when(jnp.logical_not(gets_b[j]), lambda: clear(b_recv, j))
        for i in range(2):
            both = gets_a[i] & gets_b[j]
            when(both, lambda: edge_copy(i, j).wait_recv())
            when(jnp.logical_not(both), lambda: clear(edge_recv, (j, i)))
    for j in range(2):
        mine = [b_recv[j, 0], b_recv[j, 1]]
        up = [pltpu.roll(x, (8, 64)[j], 1) for x in (edge_recv[j, 0], *mine)]
        down = [pltpu.roll(x, (64, 120)[j], 1) for x in (*mine, edge_recv[j, 1])]
        for half in range(2):
            for a in range(8):
                got = pltpu.roll(mine[half], (56 * j - a * 8) % 128, 1)
                if a == 0:
                    got = got + jnp.where(lower_half, up[half], up[half + 1])
                if a == 7:
                    got = got + jnp.where(lower_half, down[half], down[half + 1])
                start = a * 64 + 56 * j
                raw[half, start : start + 8, :] += jnp.where(node == 7 * j, got, 0.0)

    ez = lane % 8
    for half in range(2):
        for a in range(8):
            low_rows = pl.ds(a * 64, 8, stride=8)
            high_rows = pl.ds(a * 64 + 7, 8, stride=8)
            low, high = raw[half, low_rows, :], raw[half, high_rows, :]
            raw[half, low_rows, :] = low + jnp.where(ez > 0, pltpu.roll(high, 1, 1), 0.0)
            raw[half, high_rows, :] = high + jnp.where(ez < 7, pltpu.roll(low, 127, 1), 0.0)
        for part in range(4):
            rows = slice(part * 128, (part + 1) * 128)
            out[half * LANES : (half + 1) * LANES, rows] = raw[half, rows, :].T


def on_device(obs_coord, obs_resid, obs_weight, obs_dest, obs_send_slot, obs_elem, obs_slot):
    dev_count = lax.axis_size("dev")
    grp_count = lax.axis_size("grp")
    row_count = obs_resid.shape[0]
    obs_rows = row_count // LANES
    capacity = 2 * row_count // dev_count
    per_dest = capacity // LANES
    batch_rows = dev_count // BATCHES * per_dest
    vmem = pl.BlockSpec(memory_space=pltpu.VMEM)
    dma = pltpu.SemaphoreType.DMA
    regular = pltpu.SemaphoreType.REGULAR
    rows = [
        x.reshape(obs_rows, LANES)
        for x in (obs_resid, obs_weight, obs_dest, obs_send_slot, obs_elem)
    ]
    field, cost = pl.pallas_call(
        functools.partial(kernel, dev_count, grp_count, capacity),
        out_shape=(
            pltpu.VMEM((ELEM_DEV, 512), F32),
            pltpu.VMEM((1, LANES), F32),
        ),
        in_specs=[pl.BlockSpec(memory_space=pl.ANY)] * 6,
        out_specs=(vmem, vmem),
        scratch_shapes=[
            pltpu.VMEM((3, row_count), F32),
            pltpu.VMEM((obs_rows, LANES), F32),
            pltpu.VMEM((obs_rows, LANES), F32),
            pltpu.VMEM((obs_rows, LANES), jnp.int32),
            pltpu.VMEM((obs_rows, LANES), jnp.int32),
            pltpu.VMEM((obs_rows, LANES), jnp.int32),
            pltpu.VMEM((5, obs_rows, LANES), F32),
            pltpu.VMEM((dev_count, CHANNELS * per_dest + 1, LANES), F32),
            pltpu.VMEM((dev_count, CHANNELS * per_dest + 1, LANES), F32),
            pltpu.VMEM((1, LANES), F32),
            pltpu.VMEM((grp_count, 1, LANES), F32),
            pltpu.VMEM((BATCHES, 64, batch_rows, LANES), F32),
            pltpu.VMEM((BATCHES, 8 * batch_rows, LANES), F32),
            pltpu.VMEM((len(OUTER_PAIRS) * 8, ELEM_DEV), F32),
            pltpu.VMEM((len(INNER_PAIRS) * 8, ELEM_DEV), F32),
            pltpu.VMEM((2, 512, LANES), F32),
            pltpu.VMEM((2, 32, LANES), F32),
            pltpu.VMEM((2, 32, LANES), F32),
            pltpu.VMEM((2, 2, 8, LANES), F32),
            pltpu.VMEM((2, 2, 8, LANES), F32),
            pltpu.VMEM((2, 2, 8, LANES), F32),
            dma((dev_count,)),
            dma((dev_count,)),
            dma((grp_count,)),
            dma((grp_count,)),
            dma((4,)),
            dma((4,)),
            dma((2, 2)),
            dma((2, 2)),
            regular((dev_count,)),
            regular,
            regular,
        ],
        compiler_params=pltpu.CompilerParams(collective_id=0, has_side_effects=True),
    )(obs_coord, *rows)
    return field.reshape(EX, EY, EZ, 512), cost[0, 0]


def solution(mesh):
    placed = (
        P(None, ("grp", "dev")),
        P(("grp", "dev")),
        P(("grp", "dev")),
        P(("grp", "dev")),
        P(("grp", "dev")),
        P(("grp", "dev")),
        P(("grp", "dev")),
    )
    return jax.shard_map(
        on_device,
        mesh=mesh,
        in_specs=placed,
        out_specs=(P("grp", "dev", None, None), P()),
        check_vma=False,
    )
```

```python
import functools
import math

import jax
import jax.numpy as jnp
from jax import lax
from jax.experimental import pallas as pl
from jax.experimental.pallas import tpu as pltpu
from jax.sharding import PartitionSpec as P

EX = 4
EY = 8
EZ = 8
ELEM_DEV = 256
LANES = 128
CHANNELS = 5
BATCHES = 4
MESH = pl.DeviceIdType.MESH
F32 = jnp.float32
BF16 = jnp.bfloat16
F8 = jnp.float8_e4m3fn

ANCHORS = [-math.cos(math.pi * k / 7) for k in range(8)]
OUTER_PAIRS = [(a, b) for a in (0, 7) for b in range(8)]
OUTER_PAIRS += [(a, b) for a in range(1, 7) for b in (0, 7)]
INNER_PAIRS = [(a, b) for a in range(1, 7) for b in range(1, 7)]
PAIRS = OUTER_PAIRS + INNER_PAIRS
COEFS = [
    1.0 / math.prod(ANCHORS[a] - ANCHORS[m] for m in range(8) if m != a) for a in range(8)
]


def basis_values(t):
    factors = [t - p for p in ANCHORS]
    prefix = [None] * 8
    suffix = [None] * 8
    for k in range(1, 8):
        prefix[k] = factors[k - 1] if k == 1 else prefix[k - 1] * factors[k - 1]
    for k in range(6, -1, -1):
        suffix[k] = factors[k + 1] if k == 6 else suffix[k + 1] * factors[k + 1]
    basis = []
    for a in range(8):
        if a == 0:
            product = suffix[0]
        elif a == 7:
            product = prefix[7]
        else:
            product = prefix[a] * suffix[a]
        basis.append(product * COEFS[a])
    return basis


def dot_nt(left, right):
    return lax.dot_general(left, right, (((1,), (1,)), ((), ())), preferred_element_type=F32)


def halves(row):
    value = jnp.broadcast_to(row, (16, LANES))
    first = value.astype(BF16)
    return first, (value - first.astype(F32)).astype(BF16)


def one_hot(row, ids):
    tile = jnp.broadcast_to(row, (ids[0].shape[0], LANES)).astype(BF16)
    return [jnp.where(part == tile, jnp.ones((), BF16), jnp.zeros((), BF16)) for part in ids]


def spread(hot, tiles):
    return jnp.concatenate([part * tile for tile in tiles for part in hot], axis=0)


def sublane_ids(count, step=16):
    ids = lax.broadcasted_iota(jnp.int32, (step, LANES), 0)
    return [(ids + step * i).astype(F32).astype(BF16) for i in range(count // step)]


def kernel(
    dev_count, grp_count, capacity,
    coord_in, resid_in, weight_in, dest_in, slot_in, elem_in,
    out, cost,
    coord, resid, weight, dest, slot, elem, terms, send, recv,
    group_send, group_recv,
    outer, third, face_rows, inner_rows, raw, a_send, a_recv, b_send, b_recv, edge_recv,
    send_sem, recv_sem, group_send_sem, group_recv_sem,
    face_send_sem, face_recv_sem, edge_send_sem, edge_recv_sem,
    up_sem, head_sem, ready_sem,
):
    g = lax.axis_index("grp")
    d = lax.axis_index("dev")
    obs_rows = resid.shape[0]
    per_dest = capacity // LANES
    half_dev = dev_count // 2
    quarter_dev = half_dev // 2
    row_total = quarter_dev * per_dest
    batch = dev_count // BATCHES

    def when(condition, action):
        @pl.when(condition)
        def _():
            action()

    def wrapped(step_g, step_d):
        return (
            lax.rem(g + step_g + grp_count, grp_count),
            lax.rem(d + step_d + dev_count, dev_count),
        )

    loads = [
        pltpu.make_async_copy(source, sink, send_sem.at[i])
        for i, (source, sink) in enumerate(
            zip(
                (dest_in, slot_in, resid_in, weight_in, coord_in, elem_in),
                (dest, slot, resid, weight, coord, elem),
            )
        )
    ]
    for load in loads:
        load.start()

    barrier = pltpu.get_barrier_semaphore()
    def signal(semaphore, partner):
        pl.semaphore_signal(semaphore, inc=1, device_id=partner, device_id_type=MESH)

    heads = [wrapped(j, 0) for j in range(1, grp_count)]
    for p in range(dev_count):
        when(p > d, lambda: signal(barrier, (g, p)))
    for head in heads:
        when(d == 0, lambda: signal(barrier, head))
    pl.semaphore_wait(barrier, jnp.where(d == 0, len(heads), d))
    for p in range(dev_count):
        when(p < d, lambda: signal(up_sem.at[d], (g, p)))

    for load in loads:
        load.wait()

    cost_row = slice(CHANNELS * per_dest, CHANNELS * per_dest + 1)

    row_ids = sublane_ids(row_total)
    lane_ids = sublane_ids(2 * LANES, 32)
    once = jnp.minimum(d + 1, 1)

    def looped(body):
        def step(_, carry):
            body()
            return carry

        lax.fori_loop(0, once, step, 0)

    def set_terms():
        residual = resid[...]
        forcing = weight[...] * residual
        where = dest[...]
        which = slot[...]
        row = where % quarter_dev * per_dest + which // LANES
        for half in range(2):
            terms[half] = jnp.where(where // half_dev == half, row, -1).astype(F32)
        terms[2] = (where // quarter_dev % 2 * LANES + which % LANES).astype(F32)
        terms[3] = forcing
        terms[4] = elem[...].astype(F32)
        part = jnp.sum(forcing * residual, axis=0, keepdims=True)
        part = jnp.broadcast_to(0.5 * jnp.sum(part, axis=1, keepdims=True), (1, LANES))
        for p in range(dev_count):
            send[p, cost_row, :] = part

    def pack(half):
        left, right = [], []
        for r in range(obs_rows):
            columns = slice(r * LANES, (r + 1) * LANES)
            values = [halves(coord[c : c + 1, columns]) for c in range(3)]
            values.append(halves(terms[3, r : r + 1, :]))
            tiles = [high for high, _ in values]
            tiles.append(halves(terms[4, r : r + 1, :])[0])
            tiles += [low for _, low in values]
            left.append(spread(one_hot(terms[half, r : r + 1, :], row_ids), tiles))
            hot = one_hot(terms[2, r : r + 1, :], lane_ids)
            right.append(jnp.concatenate([part.astype(F8) for part in hot], axis=0))
        packed = dot_nt(jnp.concatenate(left, axis=1), jnp.concatenate(right, axis=1))
        for q in range(half_dev):
            lanes = slice(q // quarter_dev * LANES, (q // quarter_dev + 1) * LANES)
            for c in range(CHANNELS):
                start = c * row_total + q % quarter_dev * per_dest
                rows = packed[start : start + per_dest, lanes]
                if c < 4:
                    start = (c + CHANNELS) * row_total + q % quarter_dev * per_dest
                    rows = rows + packed[start : start + per_dest, lanes]
                send[half * half_dev + q, c * per_dest : (c + 1) * per_dest, :] = rows

    def data_copy(p, source):
        return pltpu.make_async_remote_copy(
            src_ref=send.at[p], dst_ref=recv.at[source],
            send_sem=send_sem.at[p], recv_sem=recv_sem.at[source],
            device_id=(g, p), device_id_type=MESH,
        )

    def group_copy(j):
        return pltpu.make_async_remote_copy(
            src_ref=group_send, dst_ref=group_recv.at[j],
            send_sem=group_send_sem.at[j], recv_sem=group_recv_sem.at[j],
            device_id=wrapped(j, 0), device_id_type=MESH,
        )

    own = d // batch

    def send_to(p):
        when(p > d, lambda: pl.semaphore_wait(up_sem.at[p], 1))
        data_copy(p, d).start()

    def pack_first():
        set_terms()
        pack(0)

    looped(pack_first)
    for p in range(half_dev):
        when(p < d, lambda: send_to(p))
    looped(lambda: pack(1))
    for p in range(half_dev, dev_count):
        when(p < d, lambda: send_to(p))
    for i in range(batch):
        when(own * batch + i > d, lambda: send_to(own * batch + i))

    def send_up(x):
        for i in range(batch):
            when(x < BATCHES, lambda: send_to(x * batch + i))

    send_up(own + 1)
    recv[d] = send[d]

    elem_ids = sublane_ids(ELEM_DEV, 32)
    rows = batch * per_dest

    def prepare(x, t, begin=0, end=batch):
        def channel(c):
            start = c * per_dest
            parts = [recv[x * batch + i, start : start + per_dest, :] for i in range(begin, end)]
            return jnp.concatenate(parts, axis=0)

        first, last = begin * per_dest, end * per_dest
        weighted = [value * channel(3) for value in basis_values(channel(0))]
        second = basis_values(channel(1))
        for c, value in enumerate(basis_values(channel(2))):
            third[t, c * rows + first : c * rows + last, :] = value
        for i, (a, b) in enumerate(PAIRS):
            outer[t, i, first:last] = weighted[a] * second[b]

    def pair_sums(x, t, groups, begin=0, end=batch):
        left, right = [], []
        for h in range(begin * per_dest, end * per_dest):
            w = third[t, pl.ds(h, 8, stride=rows), :]
            pieces = []
            for start, stop in groups:
                highs, lows = [], []
                for i in range(start, stop, 2):
                    value = jnp.concatenate([outer[t, k, h : h + 1, :] * w for k in (i, i + 1)], axis=0)
                    high = value.astype(BF16)
                    highs.append(high)
                    lows.append((value - high.astype(F32)).astype(BF16))
                pieces += highs + lows
            left.append(jnp.concatenate(pieces, axis=0))
            start = 4 * per_dest + h % per_dest
            owner = recv[x * batch + h // per_dest, start : start + 1, :]
            hot = one_hot(owner, elem_ids)
            right.append(jnp.concatenate([part.astype(F8) for part in hot], axis=0))
        total = dot_nt(jnp.concatenate(left, axis=1), jnp.concatenate(right, axis=1))
        sums, row = [], 0
        for start, stop in groups:
            count = (stop - start) * 8
            sums.append(total[row : row + count] + total[row + count : row + 2 * count])
            row += 2 * count
        return sums

    faces, inners = (0, len(OUTER_PAIRS)), (len(OUTER_PAIRS), len(PAIRS))

    def arrive(source):
        data_copy(source, source).wait_recv()

    for i in range(batch):
        when(own * batch + i != d, lambda: arrive(own * batch + i))

    def first_sums():
        prepare(own, 0)
        face_rows[...], inner_rows[...] = pair_sums(own, 0, (faces, inners))

    looped(first_sums)

    for j in range(2, BATCHES):
        send_up(own + j)
    for head in heads:
        when(d == 0, lambda: signal(head_sem, head))

    def batch_of(t):
        early = own < BATCHES // 2
        turn = jnp.where(early, own, BATCHES - 1 - own)
        x = t - 1 + (t > turn).astype(jnp.int32)
        return jnp.where(early, x, BATCHES - 1 - x)

    def from_batch(t):
        x = batch_of(t)
        for i in range(batch):
            arrive(x * batch + i)
        prepare(x, t)
        return x

    def tell_ready():
        pl.semaphore_wait(head_sem, len(heads))
        for p in range(1, dev_count):
            signal(ready_sem, (g, p))

    def only_faces(t, carry):
        face_rows[...] += pair_sums(from_batch(t), t, (faces,))[0]
        when((d == 0) & (t == 1), tell_ready)
        return carry

    def only_inner(t, carry):
        inner_rows[...] += pair_sums(batch_of(t), t, (inners,))[0]
        return carry

    lax.fori_loop(1, BATCHES - 1, only_faces, 0)
    last = from_batch(BATCHES - 1)
    group_cost = recv[0, cost_row, :]
    for i in range(1, dev_count):
        group_cost = group_cost + recv[i, cost_row, :]
    group_send[...] = group_cost
    when(d > 0, lambda: pl.semaphore_wait(ready_sem, 1))
    for j in range(1, grp_count):
        group_copy(j).start()

    def place(value, pairs):
        for i, (a, b) in enumerate(pairs):
            start = a * 64 + b * 8
            for half in range(2):
                lanes = slice(half * LANES, (half + 1) * LANES)
                raw[half, start : start + 8, :] = value[i * 8 : i * 8 + 8, lanes]

    def last_faces():
        place(face_rows[...] + pair_sums(last, BATCHES - 1, (faces,))[0], OUTER_PAIRS)

    looped(last_faces)

    lane = lax.broadcasted_iota(jnp.int32, (1, LANES), 1)
    lower_half = lane < 64
    node = (lane // 8) % 8
    for half in range(2):
        up = pltpu.roll(raw[half, 56:64, :], 72, 1)
        down = raw[half, 0:8, :]
        for a in range(1, 8):
            high = raw[half, a * 64 + 56 : a * 64 + 64, :]
            low = raw[half, a * 64 : a * 64 + 8, :]
            up = jnp.where(node == a, pltpu.roll(high, (a * 8 + 72) % 128, 1), up)
            down = jnp.where(node == a, pltpu.roll(low, a * 8, 1), down)
        b_send[0, half] = up
        b_send[1, half] = down

    steps = (1, -1)

    def face_copy(i):
        if i < 2:
            source, sink, target = a_send.at[i], a_recv.at[i], wrapped(steps[i], 0)
        else:
            source, sink, target = b_send.at[i - 2], b_recv.at[i - 2], wrapped(0, steps[i - 2])
        return pltpu.make_async_remote_copy(
            src_ref=source, dst_ref=sink,
            send_sem=face_send_sem.at[i], recv_sem=face_recv_sem.at[i],
            device_id=target, device_id_type=MESH,
        )

    def edge_copy(i, j):
        return pltpu.make_async_remote_copy(
            src_ref=b_send.at[j, 1 - i], dst_ref=edge_recv.at[j, i],
            send_sem=edge_send_sem.at[j, i], recv_sem=edge_recv_sem.at[j, i],
            device_id=wrapped(steps[i], steps[j]), device_id_type=MESH,
        )

    sends_a, sends_b = (g < grp_count - 1, g > 0), (d < dev_count - 1, d > 0)
    gets_a, gets_b = (g > 0, g < grp_count - 1), (d > 0, d < dev_count - 1)

    def clear(ref, i):
        ref[i] = jnp.zeros_like(ref[i])

    for i in (1, 0):
        for j in range(2):
            when(sends_a[i] & sends_b[j], lambda: edge_copy(i, j).start())
    block = raw[1, 448:512, :]
    a_send[0] = jnp.where(lower_half, pltpu.roll(block[0:32], 64, 1), block[32:64])
    block = raw[0, 0:64, :]
    a_send[1] = jnp.where(lower_half, block[0:32], pltpu.roll(block[32:64], 64, 1))
    for i in (1, 0):
        when(sends_a[i], lambda: face_copy(i).start())
        when(sends_b[i], lambda: face_copy(2 + i).start())

    lax.fori_loop(1, BATCHES, only_inner, 0)
    place(inner_rows[...], INNER_PAIRS)

    low_rows, high_rows = slice(0, 64), slice(448, 512)
    low = [raw[half, low_rows, :] for half in range(2)]
    high = [raw[half, high_rows, :] for half in range(2)]
    low_rolled = [pltpu.roll(x, 64, 1) for x in low]
    high_rolled = [pltpu.roll(x, 64, 1) for x in high]
    raw[0, low_rows, :] = low[0] + jnp.where(lower_half, 0.0, high_rolled[0])
    raw[1, low_rows, :] = low[1] + jnp.where(lower_half, high_rolled[0], high_rolled[1])
    raw[0, high_rows, :] = high[0] + jnp.where(lower_half, low_rolled[0], low_rolled[1])
    raw[1, high_rows, :] = high[1] + jnp.where(lower_half, low_rolled[1], 0.0)

    def from_below(high):
        return jnp.where(node == 0, 0.0, pltpu.roll(high, 8, 1))

    def from_above(low):
        return jnp.where(node == 7, 0.0, pltpu.roll(low, 120, 1))

    for half in range(2):
        for a in range(8):
            low_rows, high_rows = slice(a * 64, a * 64 + 8), slice(a * 64 + 56, a * 64 + 64)
            low, high = raw[half, low_rows, :], raw[half, high_rows, :]
            raw[half, low_rows, :] = low + from_below(high)
            raw[half, high_rows, :] = high + from_above(low)

    all_cost = group_send[...]
    for j in range(1, grp_count):
        group_copy(j).wait_recv()
        all_cost = all_cost + group_recv[j]
    cost[...] = all_cost

    for p in range(dev_count):
        when(p != d, lambda: data_copy(p, p).wait_send())
    for j in range(1, grp_count):
        group_copy(j).wait_send()
    for i in range(2):
        when(sends_a[i], lambda: face_copy(i).wait_send())
        when(sends_b[i], lambda: face_copy(2 + i).wait_send())
        for j in range(2):
            when(sends_a[i] & sends_b[j], lambda: edge_copy(i, j).wait_send())

    for i in range(2):
        when(gets_a[i], lambda: face_copy(i).wait_recv())
        when(jnp.logical_not(gets_a[i]), lambda: clear(a_recv, i))
    for i in range(2):
        got = a_recv[i]
        far = pltpu.roll(got, 64, 1)
        start = i * 448
        if i == 0:
            keep, low, high = lower_half, got[0:8], pltpu.roll(got[24:32], 72, 1)
            low = pltpu.roll(low, 120, 1)
            got = jnp.concatenate([got, far], axis=0)
        else:
            keep, low, high = jnp.logical_not(lower_half), pltpu.roll(got[0:8], 56, 1), got[24:32]
            high = pltpu.roll(high, 8, 1)
            got = jnp.concatenate([far, got], axis=0)
        got = jnp.where(keep, got, 0.0)
        raw[i, start : start + 8, :] += got[0:8] + jnp.where(keep & (node > 0), high, 0.0)
        raw[i, start + 8 : start + 56, :] += got[8:56]
        raw[i, start + 56 : start + 64, :] += got[56:64] + jnp.where(keep & (node < 7), low, 0.0)

    for j in range(2):
        when(gets_b[j], lambda: face_copy(2 + j).wait_recv())
        when(jnp.logical_not(gets_b[j]), lambda: clear(b_recv, j))
        for i in range(2):
            both = gets_a[i] & gets_b[j]
            when(both, lambda: edge_copy(i, j).wait_recv())
            when(jnp.logical_not(both), lambda: clear(edge_recv, (j, i)))
    for j in range(2):
        mine = [b_recv[j, 0], b_recv[j, 1]]
        up = [pltpu.roll(x, (8, 64)[j], 1) for x in (edge_recv[j, 0], *mine)]
        down = [pltpu.roll(x, (64, 120)[j], 1) for x in (*mine, edge_recv[j, 1])]
        for half in range(2):
            for a in range(8):
                got = pltpu.roll(mine[half], (56 * j - a * 8) % 128, 1)
                if a == 0:
                    got = got + jnp.where(lower_half, up[half], up[half + 1])
                if a == 7:
                    got = got + jnp.where(lower_half, down[half], down[half + 1])
                start = a * 64 + 56 * j
                raw[half, start : start + 8, :] += jnp.where(node == 7 * j, got, 0.0)

    ez = lane % 8
    for half in range(2):
        for a in range(8):
            low_rows = pl.ds(a * 64, 8, stride=8)
            high_rows = pl.ds(a * 64 + 7, 8, stride=8)
            low, high = raw[half, low_rows, :], raw[half, high_rows, :]
            raw[half, low_rows, :] = low + jnp.where(ez > 0, pltpu.roll(high, 1, 1), 0.0)
            raw[half, high_rows, :] = high + jnp.where(ez < 7, pltpu.roll(low, 127, 1), 0.0)
        for part in range(4):
            rows = slice(part * 128, (part + 1) * 128)
            out[half * LANES : (half + 1) * LANES, rows] = raw[half, rows, :].T


def on_device(obs_coord, obs_resid, obs_weight, obs_dest, obs_send_slot, obs_elem, obs_slot):
    dev_count = lax.axis_size("dev")
    grp_count = lax.axis_size("grp")
    row_count = obs_resid.shape[0]
    obs_rows = row_count // LANES
    capacity = 2 * row_count // dev_count
    per_dest = capacity // LANES
    batch_rows = dev_count // BATCHES * per_dest
    vmem = pl.BlockSpec(memory_space=pltpu.VMEM)
    dma = pltpu.SemaphoreType.DMA
    regular = pltpu.SemaphoreType.REGULAR
    rows = [
        x.reshape(obs_rows, LANES)
        for x in (obs_resid, obs_weight, obs_dest, obs_send_slot, obs_elem)
    ]
    field, cost = pl.pallas_call(
        functools.partial(kernel, dev_count, grp_count, capacity),
        out_shape=(
            pltpu.VMEM((ELEM_DEV, 512), F32),
            pltpu.VMEM((1, LANES), F32),
        ),
        in_specs=[pl.BlockSpec(memory_space=pl.ANY)] * 6,
        out_specs=(vmem, vmem),
        scratch_shapes=[
            pltpu.VMEM((3, row_count), F32),
            pltpu.VMEM((obs_rows, LANES), F32),
            pltpu.VMEM((obs_rows, LANES), F32),
            pltpu.VMEM((obs_rows, LANES), jnp.int32),
            pltpu.VMEM((obs_rows, LANES), jnp.int32),
            pltpu.VMEM((obs_rows, LANES), jnp.int32),
            pltpu.VMEM((5, obs_rows, LANES), F32),
            pltpu.VMEM((dev_count, CHANNELS * per_dest + 1, LANES), F32),
            pltpu.VMEM((dev_count, CHANNELS * per_dest + 1, LANES), F32),
            pltpu.VMEM((1, LANES), F32),
            pltpu.VMEM((grp_count, 1, LANES), F32),
            pltpu.VMEM((BATCHES, 64, batch_rows, LANES), F32),
            pltpu.VMEM((BATCHES, 8 * batch_rows, LANES), F32),
            pltpu.VMEM((len(OUTER_PAIRS) * 8, ELEM_DEV), F32),
            pltpu.VMEM((len(INNER_PAIRS) * 8, ELEM_DEV), F32),
            pltpu.VMEM((2, 512, LANES), F32),
            pltpu.VMEM((2, 32, LANES), F32),
            pltpu.VMEM((2, 32, LANES), F32),
            pltpu.VMEM((2, 2, 8, LANES), F32),
            pltpu.VMEM((2, 2, 8, LANES), F32),
            pltpu.VMEM((2, 2, 8, LANES), F32),
            dma((dev_count,)),
            dma((dev_count,)),
            dma((grp_count,)),
            dma((grp_count,)),
            dma((4,)),
            dma((4,)),
            dma((2, 2)),
            dma((2, 2)),
            regular((dev_count,)),
            regular,
            regular,
        ],
        compiler_params=pltpu.CompilerParams(collective_id=0, has_side_effects=True),
    )(obs_coord, *rows)
    return field.reshape(EX, EY, EZ, 512), cost[0, 0]


def solution(mesh):
    placed = (
        P(None, ("grp", "dev")),
        P(("grp", "dev")),
        P(("grp", "dev")),
        P(("grp", "dev")),
        P(("grp", "dev")),
        P(("grp", "dev")),
        P(("grp", "dev")),
    )
    return jax.shard_map(
        on_device,
        mesh=mesh,
        in_specs=placed,
        out_specs=(P("grp", "dev", None, None), P()),
        check_vma=False,
    )
```
